8 devices in a mesh: dp: 1 (over z), tp: 8 (over y, x, core).
Axes of the slice: x: 2, y: 2, z: 1, core: 2. Of those that a mesh axis runs over, the one named last changes fastest.
Arguments:
- hidden: bfloat16 [4096, 1280], P(('dp', 'tp'))
- ln_gamma: float32 [1280], replicated
- ln_beta: float32 [1280], replicated
- out_embed: bfloat16 [51200, 1280], P('tp')
- vocab_valid: int32 [51200], P('tp')
- targets: int32 [4096], P(('dp', 'tp'))
- loss_mask: int32 [4096], P(('dp', 'tp'))
Outputs:
- output 1: float32 [4096], P(('dp', 'tp'))
- output 2: float32 [1], P('dp')
- output 3: bfloat16 [4096, 1280], P(('dp', 'tp'))
- output 4: float32 [51200, 1280], P(('dp', 'tp'))
- output 5: float32 [1280], P('dp')
- output 6: float32 [1280], P('dp')
All inputs are finite; a program needn't handle non-finite values.
Results may differ from the reference program's by a relative error of at most 0.001.
Values are sent between devices in bfloat16 or wider.
A program may use at most 1 GiB of HBM per device.

```python
import jax
import jax.numpy as jnp
from jax import lax

GROUP_SIZE = 8
TOKENS_DEV = 512
MODEL_DIM = 1280
VOCAB_SIZE = 50257

SEQ_LEN = GROUP_SIZE * TOKENS_DEV
PAD_UNIT = 128 * GROUP_SIZE
VOCAB_PAD = (VOCAB_SIZE + PAD_UNIT - 1) // PAD_UNIT * PAD_UNIT
SHARD_VOCAB = VOCAB_PAD // GROUP_SIZE
DROP_COUNT = VOCAB_SIZE // 8
LN_EPS = 1e-5


def setup_inputs(seed: int = 0, part: int = 0) -> dict:
    base_key = jax.random.key(seed)
    k_gamma, k_beta, k_embed, k_perm = jax.random.split(base_key, 4)
    k_hidden, k_start, k_end, k_keep, k_target = jax.random.split(jax.random.fold_in(base_key, part), 5)
    hidden = jax.random.normal(k_hidden, (SEQ_LEN, MODEL_DIM), jnp.float32).astype(jnp.bfloat16)
    ln_gamma = 1.0 + 0.3 * jax.random.normal(k_gamma, (MODEL_DIM,), jnp.float32)
    ln_beta = 0.3 * jax.random.normal(k_beta, (MODEL_DIM,), jnp.float32)
    embed_scale = 2.5 * MODEL_DIM ** -0.5
    out_embed = (embed_scale * jax.random.normal(k_embed, (VOCAB_PAD, MODEL_DIM), jnp.float32)).astype(jnp.bfloat16)
    perm_ids = jax.random.permutation(k_perm, VOCAB_SIZE)
    vocab_ids = jnp.arange(VOCAB_PAD)
    vocab_valid = (vocab_ids < VOCAB_SIZE).astype(jnp.int32).at[perm_ids[:DROP_COUNT]].set(0)
    allowed_ids = perm_ids[DROP_COUNT:]
    pick_idx = jax.random.randint(k_target, (SEQ_LEN,), 0, VOCAB_SIZE - DROP_COUNT)
    targets = allowed_ids[pick_idx].astype(jnp.int32)
    positions = jnp.arange(SEQ_LEN)
    half_shard = TOKENS_DEV // 2
    start_pos = jax.random.randint(k_start, (), 0, half_shard + 1)
    end_pos = SEQ_LEN - jax.random.randint(k_end, (), 0, half_shard + 1)
    keep_tok = (jax.random.randint(k_keep, (SEQ_LEN,), 0, 4) != 0) | (positions == SEQ_LEN // 2)
    loss_mask = ((positions >= start_pos) & (positions < end_pos) & keep_tok).astype(jnp.int32)
    return {"hidden": hidden, "ln_gamma": ln_gamma, "ln_beta": ln_beta, "out_embed": out_embed, "vocab_valid": vocab_valid, "targets": targets, "loss_mask": loss_mask}


def layer_norm(hidden32, ln_gamma, ln_beta):
    row_mean = jnp.mean(hidden32, axis=-1, keepdims=True)
    centered = hidden32 - row_mean
    row_var = jnp.mean(centered * centered, axis=-1, keepdims=True)
    return centered * lax.rsqrt(row_var + LN_EPS) * ln_gamma + ln_beta


def reference(hidden, ln_gamma, ln_beta, out_embed, vocab_valid, targets, loss_mask):
    normed, ln_vjp = jax.vjp(layer_norm, hidden.astype(jnp.float32), ln_gamma, ln_beta)
    x_all = normed.astype(jnp.bfloat16)
    allowed = vocab_valid[None, :] > 0
    vocab_ids = jnp.arange(VOCAB_PAD)
    x_blocks = x_all.reshape(GROUP_SIZE, TOKENS_DEV, MODEL_DIM)
    tgt_blocks = targets.reshape(GROUP_SIZE, TOKENS_DEV)

    def token_block(block_args):
        x_blk, tgt_blk = block_args
        logits = jnp.dot(x_blk, out_embed.T, preferred_element_type=jnp.float32)
        log_norm = jax.nn.logsumexp(jnp.where(allowed, logits, -jnp.inf), axis=-1)
        picked = jnp.sum(jnp.where(vocab_ids[None, :] == tgt_blk[:, None], logits, 0.0), axis=-1)
        return log_norm, picked

    log_norm, picked = lax.map(token_block, (x_blocks, tgt_blocks))
    log_norm = log_norm.reshape(SEQ_LEN)
    picked = picked.reshape(SEQ_LEN)
    weight = loss_mask.astype(jnp.float32)
    tok_count = jnp.sum(weight)
    tok_loss = (log_norm - picked) * weight
    mean_loss = jnp.sum(tok_loss) / tok_count
    tok_scale = weight / tok_count

    embed_shards = out_embed.reshape(GROUP_SIZE, SHARD_VOCAB, MODEL_DIM)
    valid_shards = vocab_valid.reshape(GROUP_SIZE, SHARD_VOCAB)
    shard_start = jnp.arange(GROUP_SIZE) * SHARD_VOCAB

    def vocab_block(dx_acc, block_args):
        emb_blk, valid_blk, offset = block_args
        logits = jnp.dot(x_all, emb_blk.T, preferred_element_type=jnp.float32)
        soft_probs = jnp.where(valid_blk[None, :] > 0, jnp.exp(logits - log_norm[:, None]), 0.0)
        target_hit = (offset + jnp.arange(SHARD_VOCAB))[None, :] == targets[:, None]
        d_logits = ((soft_probs - target_hit.astype(jnp.float32)) * tok_scale[:, None]).astype(jnp.bfloat16)
        d_emb = jnp.dot(d_logits.T, x_all, preferred_element_type=jnp.float32)
        dx_acc = dx_acc + jnp.dot(d_logits, emb_blk, preferred_element_type=jnp.float32)
        return dx_acc, d_emb

    dx_all, d_embed = lax.scan(vocab_block, jnp.zeros((SEQ_LEN, MODEL_DIM), jnp.float32), (embed_shards, valid_shards, shard_start))
    d_embed = d_embed.reshape(VOCAB_PAD, MODEL_DIM)
    d_hidden, d_gamma, d_beta = ln_vjp(dx_all)
    return tok_loss, mean_loss.reshape(1), d_hidden.astype(jnp.bfloat16), d_embed, d_gamma, d_beta
```

```python
import functools

import jax
import jax.numpy as jnp
from jax import lax
from jax.experimental import pallas as pl
from jax.experimental.pallas import tpu as pltpu
from jax.sharding import PartitionSpec as P

LN_EPS = 1e-5
LANES = 128
NB = 5
LAG = NB + 1
LOW = float(jnp.finfo(jnp.float32).min)
MESH = pl.DeviceIdType.MESH
NT = (((1,), (1,)), ((), ()))


def _spread(row):
    return jnp.broadcast_to(row, (LANES, LANES)).T


def fused_kernel(
    hid_ref, gam_ref, bet_ref, emb_hbm, valid_ref, tm_ref,
    dz_hbm, xall_hbm, dh_ref, loss_ref, gb_ref,
    xv, ev, ring, acc, dzb, bias, m_sc, s_sc, p_sc, t1_sc, t2_sc, lse_sc, w_sc,
    tm_all, st_send, st_recv, r0, r1, r2, gb_send, gb_recv,
    e_sem, ag_send, ag_recv, fw_send, tm_send, tm_recv, st_ssem, st_rsem,
    s0, q0, s1, q1, s2, q2, free0, free1, free2, gb_ssem, gb_rsem, dz_sem, x_sem,
):
    nc, tok, dim = xv.shape
    vb = ev.shape[1]
    own = tok // 8
    half = tok // 2
    me = lax.axis_index("tp")
    core = lax.rem(me, 2)
    xc = lax.rem(me // 2, 2)
    yc = me // 4

    def dev(y, x, k):
        return y * 4 + x * 2 + k

    def slot_of(y, x, k):
        return k * 4 + y * 2 + x

    sib = dev(yc, xc, 1 - core)
    xn = dev(yc, 1 - xc, core)
    yn = dev(1 - yc, xc, core)
    dn = dev(1 - yc, 1 - xc, core)
    remote = ((xn, slot_of(yc, 1 - xc, core)), (yn, slot_of(1 - yc, xc, core)), (dn, slot_of(1 - yc, 1 - xc, core)))
    my_slot = slot_of(yc, xc, core)
    first_n = jnp.where(core == 0, xn, yn)
    second_n = jnp.where(core == 0, yn, xn)

    def rcopy(src, dst, ssem, rsem, to):
        return pltpu.make_async_remote_copy(src_ref=src, dst_ref=dst, send_sem=ssem, recv_sem=rsem, device_id={"tp": to}, device_id_type=MESH)

    def rows(slot):
        return pl.ds(pl.multiple_of(slot * own, own), own)

    for j in range(NB):
        pltpu.make_async_copy(emb_hbm.at[j], ev.at[j], e_sem.at[j]).start()

    barrier = pltpu.get_barrier_semaphore()
    for k in range(1, 8):
        pl.semaphore_signal(barrier, inc=1, device_id={"tp": lax.rem(me + k, 8)}, device_id_type=MESH)
    pl.semaphore_wait(barrier, 7)

    tm_all[me] = tm_ref[...]

    def tm_copy(k):
        return rcopy(tm_ref, tm_all.at[me], tm_send.at[k], tm_recv.at[k], lax.rem(me + k, 8))

    for k in range(1, 8):
        tm_copy(k).start()

    def ln(c):
        h = hid_ref[pl.ds(pl.multiple_of(c * own, own), own), :].astype(jnp.float32)
        cen = h - jnp.mean(h, axis=1, keepdims=True)
        rstd = lax.rsqrt(jnp.mean(cen * cen, axis=1, keepdims=True) + LN_EPS)
        return cen * rstd, rstd

    def ag_copy(c, k):
        r = xv.at[c, rows(my_slot)]
        return rcopy(r, r, ag_send.at[c, k], ag_recv.at[c, k], (xn, yn, dn, sib)[k])

    def fw_copy(c, k):
        r = xv.at[c, rows(remote[k][1])]
        return rcopy(r, r, fw_send.at[c, k], ag_recv.at[c, 4 + k], sib)

    def ln_body(c, _):
        xhat, _r = ln(c)
        xv[c, rows(my_slot), :] = (xhat * gam_ref[...] + bet_ref[...]).astype(jnp.bfloat16)

        @pl.when(c >= 1)
        def _():
            for k in (2, 0, 1, 3):
                ag_copy(c - 1, k).start()
        return 0

    lax.fori_loop(0, nc, ln_body, 0)
    for k in (2, 0, 1, 3):
        ag_copy(nc - 1, k).start()

    bias[...] = jnp.where(valid_ref[...] > 0, 0.0, -jnp.inf)
    gb_send[...] = jnp.zeros_like(gb_send)

    def recv_remote(c):
        for k in range(3):
            ag_copy(c, k).wait_recv()

    def forward(c):
        recv_remote(c)
        for k in range(3):
            fw_copy(c, k).start()

    for k in range(1, 8):
        tm_copy(k).wait_recv()
    count = jnp.zeros((8, LANES), jnp.float32)
    for d in range(8):
        count = count + tm_all[d, 1]
    count = jnp.sum(jnp.sum(count, axis=1, keepdims=True), axis=0, keepdims=True)
    inv_n = 1.0 / count

    def tm_rows(c, which):
        out = []
        for q in range(4):
            k, y = q // 2, q % 2
            out.append(tm_all[dev(y, 0, k), which, pl.ds(c, 1), :] + tm_all[dev(y, 1, k), which, pl.ds(c, 1), :])
        return out

    forward(0)
    lane = lax.broadcasted_iota(jnp.int32, (tok, LANES), 1)

    def st_copy(c, k):
        return rcopy(st_send.at[c], st_recv.at[c, me], st_ssem.at[c, k], st_rsem.at[c, k], lax.rem(me + k, 8))

    def send_stats(c):
        li = lax.broadcasted_iota(jnp.int32, (LANES, LANES), 1)
        for q in range(4):
            r = pl.ds(q * LANES, LANES)
            m = m_sc[r]
            mx = jnp.max(m, axis=1, keepdims=True)
            s = jnp.sum(s_sc[r] * jnp.exp(m - mx), axis=1, keepdims=True)
            p = jnp.sum(p_sc[r], axis=1, keepdims=True)
            v = jnp.where(li == 0, mx, jnp.where(li == 1, s, p))
            st_send[c, q] = v.T[:8]
        st_recv[c, me] = st_send[c]
        for k in range(1, 8):
            st_copy(c, k).start()

    def use_stats(c):
        for k in range(1, 8):
            st_copy(c, k).wait_recv()
        tg = tm_rows(c, 0)
        mk = tm_rows(c, 1)
        for q in range(4):
            mx = st_recv[c, 0, q, 0:1]
            for d in range(1, 8):
                mx = jnp.maximum(mx, st_recv[c, d, q, 0:1])
            s = jnp.zeros_like(mx)
            p = jnp.zeros_like(mx)
            for d in range(8):
                s = s + st_recv[c, d, q, 1:2] * jnp.exp(st_recv[c, d, q, 0:1] - mx)
                p = p + st_recv[c, d, q, 2:3]
            lse = mx + jnp.log(s)
            loss_ref[c, pl.ds(q, 1), :] = (lse - p) * mk[q]
            r = pl.ds(q * LANES, LANES)
            lse_sc[r] = _spread(lse)
            w_sc[r] = _spread(mk[q] * inv_n)
            t2_sc[r] = _spread(tg[q]).astype(jnp.int32)

    def begin_chunk(c):
        for k in range(3, 7):
            if k == 3:
                ag_copy(c, 3).wait_recv()
            else:
                fw_copy(c, k - 4).wait_recv()
        pltpu.make_async_copy(xv.at[c], xall_hbm.at[c], x_sem.at[c]).start()
        m_sc[...] = jnp.full(m_sc.shape, LOW, jnp.float32)
        s_sc[...] = jnp.zeros_like(s_sc)
        p_sc[...] = jnp.zeros_like(p_sc)
        tg = tm_rows(c, 0)
        for q in range(4):
            t1_sc[pl.ds(q * LANES, LANES)] = _spread(tg[q]).astype(jnp.int32)

    def first_src(b):
        return jnp.where(core == 0, b * 2 + (1 - xc), (1 - yc) * 2 + b)

    def first_keep(b):
        return jnp.where(core == 0, b * 2 + xc, yc * 2 + b)

    own2 = jnp.where(core == 0, yc, xc)

    def c0(c):
        a = lax.rem(c, 2)
        return rcopy(acc.at[a, pl.ds(pl.multiple_of((1 - core) * half, half), half)], r0.at[a], s0.at[a], q0.at[a], sib)

    def c1(c, b):
        a = lax.rem(c, 2)
        return rcopy(r0.at[a, rows(first_src(b))], r1.at[a, b], s1.at[a, b], q1.at[a, b], first_n)

    def c2(c):
        a = lax.rem(c, 2)
        return rcopy(r1.at[a, 1 - own2], r2.at[a], s2.at[a], q2.at[a], second_n)

    def stage0(c):
        @pl.when(c >= 2)
        def _():
            pl.semaphore_wait(free0, 1)
        c0(c).start()

    def stage1(c):
        a = lax.rem(c, 2)
        c0(c).wait()
        r0[a] = r0[a] + acc[a, pl.ds(pl.multiple_of(core * half, half), half)]

        @pl.when(c >= 2)
        def _():
            pl.semaphore_wait(free1, 1)
        for b in range(2):
            c1(c, b).start()

    def stage2(c):
        a = lax.rem(c, 2)
        for b in range(2):
            c1(c, b).wait()
        for b in range(2):
            r1[a, b] = r1[a, b] + r0[a, rows(first_keep(b))]

        @pl.when(c >= 2)
        def _():
            pl.semaphore_wait(free2, 1)
        c2(c).start()

        @pl.when(c < nc - 2)
        def _():
            pl.semaphore_signal(free0, inc=1, device_id={"tp": sib}, device_id_type=MESH)

    def stage3(c):
        a = lax.rem(c, 2)
        c2(c).wait()
        dy = r1[a, own2] + r2[a]

        @pl.when(c < nc - 2)
        def _():
            pl.semaphore_signal(free1, inc=1, device_id={"tp": first_n}, device_id_type=MESH)
            pl.semaphore_signal(free2, inc=1, device_id={"tp": second_n}, device_id_type=MESH)
        xhat, rstd = ln(c)
        gb_send[0:1] += jnp.sum(dy * xhat, axis=0, keepdims=True)
        gb_send[1:2] += jnp.sum(dy, axis=0, keepdims=True)
        dxh = dy * gam_ref[...]
        m1 = jnp.mean(dxh, axis=1, keepdims=True)
        m2 = jnp.mean(dxh * xhat, axis=1, keepdims=True)
        dh_ref[pl.ds(pl.multiple_of(c * own, own), own), :] = (rstd * (dxh - m1 - xhat * m2)).astype(jnp.bfloat16)

    base = me * (NB * vb)

    def dz_copy(t):
        a = lax.rem(t, 2)
        t2 = t - LAG
        return pltpu.make_async_copy(dzb.at[a], dz_hbm.at[lax.rem(t2, NB), pl.ds(pl.multiple_of((t2 // NB) * tok, tok), tok)], dz_sem.at[a])

    def compute(t, do1, do2):
        slot = lax.rem(t, LAG)
        a2 = lax.rem(t, 2)
        if do2:
            t2 = t - LAG
            j2 = lax.rem(t2, NB)
            tr = t2_sc[...] - (base + j2 * vb)
            for k in range(vb // LANES):
                col = k * LANES
                p = jnp.exp(ring[slot, :, pl.ds(col, LANES)] - lse_sc[...])
                p = jnp.where(tr == lane + col, p - 1.0, p) * w_sc[...]
                dzb[a2, :, pl.ds(col, LANES)] = p.astype(jnp.bfloat16)
        if do1:
            j1 = lax.rem(t, NB)
            tr = t1_sc[...] - (base + j1 * vb)
            z = lax.dot_general(xv[t // NB], ev[j1], NT, preferred_element_type=jnp.float32) + bias[j1]
            ring[slot] = z
            zs = [z[:, k * LANES:(k + 1) * LANES] for k in range(vb // LANES)]
            m0 = m_sc[...]
            m = m0
            for q in zs:
                m = jnp.maximum(m, q)
            s = s_sc[...] * jnp.exp(m0 - m)
            pk = p_sc[...]
            for k, q in enumerate(zs):
                s = s + jnp.exp(q - m)
                pk = pk + jnp.where(tr == lane + k * LANES, q, 0.0)
            m_sc[...] = m
            s_sc[...] = s
            p_sc[...] = pk
        if do2:
            a = lax.rem(t2 // NB, 2)
            acc[a] = acc[a] + jnp.dot(dzb[a2], ev[j2], preferred_element_type=jnp.float32)

    def step(t, do1, do2):
        ph = lax.rem(t, NB)
        if do1:
            @pl.when(ph == 0)
            def _():
                begin_chunk(t // NB)

            @pl.when((ph == 2) & (t // NB + 1 < nc))
            def _():
                forward(t // NB + 1)

            @pl.when(t < NB)
            def _():
                pltpu.make_async_copy(emb_hbm.at[ph], ev.at[ph], e_sem.at[ph]).wait()
        if do2:
            @pl.when((ph == 1) & (t >= 11))
            def _():
                stage0((t - 11) // NB)

            @pl.when(ph == 1)
            def _():
                c = (t - LAG) // NB
                use_stats(c)
                acc[lax.rem(c, 2)] = jnp.zeros((tok, dim), jnp.float32)

            @pl.when((ph == 2) & (t >= 17))
            def _():
                stage3((t - 17) // NB)

            @pl.when((ph == 2) & (t >= 12))
            def _():
                stage1((t - 12) // NB)

            @pl.when((ph == 0) & (t >= 15))
            def _():
                stage2((t - 15) // NB)

            @pl.when(t >= LAG + 2)
            def _():
                dz_copy(t - 2).wait()
        compute(t, do1, do2)
        if do2:
            dz_copy(t).start()
        if do1:
            @pl.when(ph == NB - 1)
            def _():
                send_stats(t // NB)

    def loop(lo, hi, do1, do2):
        def body(t, _):
            step(t, do1, do2)
            return 0
        lax.fori_loop(lo, hi, body, 0)

    total = NB * nc
    loop(0, LAG, True, False)
    loop(LAG, total, True, True)
    loop(total, total + LAG, False, True)

    last = nc - 1
    stage0(last)
    stage3(last - 1)
    stage1(last)
    stage2(last)
    stage3(last)

    def gb_copy(k):
        return rcopy(gb_send, gb_recv.at[me], gb_ssem.at[k], gb_rsem.at[k], lax.rem(me + k, 8))

    for k in range(1, 8):
        gb_copy(k).start()
    gb_recv[me] = gb_send[...]
    for t in (total + LAG - 2, total + LAG - 1):
        dz_copy(t).wait()

    def drain(c, _):
        for k in range(4):
            ag_copy(c, k).wait_send()
        for k in range(3):
            fw_copy(c, k).wait_send()
        for k in range(1, 8):
            st_copy(c, k).wait_send()
        pltpu.make_async_copy(xv.at[c], xall_hbm.at[c], x_sem.at[c]).wait()
        return 0

    lax.fori_loop(0, nc, drain, 0)
    for k in range(1, 8):
        tm_copy(k).wait_send()
        gb_copy(k).wait()
    tot = gb_recv[0]
    for d in range(1, 8):
        tot = tot + gb_recv[d]
    gb_ref[...] = tot
    gb_ref[2:3] = jnp.broadcast_to(count, (1, dim))


def fused(hidden, gamma, beta, embed, valid, tm):
    tok, dim = hidden.shape
    nc = 8
    own = tok // nc
    vb = embed.shape[0] // NB
    full = own * 8
    f32, bf16 = jnp.float32, jnp.bfloat16
    sds = jax.ShapeDtypeStruct
    vmem = pl.BlockSpec(memory_space=pltpu.VMEM)
    hbm = pl.BlockSpec(memory_space=pl.ANY)
    col = pltpu.VMEM((full, LANES), f32)
    coli = pltpu.VMEM((full, LANES), jnp.int32)
    dma, reg = pltpu.SemaphoreType.DMA, pltpu.SemaphoreType.REGULAR
    flops = 4 * full * nc * embed.shape[0] * dim
    return pl.pallas_call(
        fused_kernel,
        out_shape=(
            sds((NB, nc * full, vb), bf16),
            sds((nc, full, dim), bf16),
            sds((tok, dim), bf16),
            sds((nc, 4, LANES), f32),
            sds((8, dim), f32),
        ),
        in_specs=[vmem, vmem, vmem, hbm, vmem, vmem],
        out_specs=(hbm, hbm, vmem, vmem, vmem),
        scratch_shapes=[
            pltpu.VMEM((nc, full, dim), bf16),
            pltpu.VMEM((NB, vb, dim), bf16),
            pltpu.VMEM((LAG, full, vb), f32),
            pltpu.VMEM((2, full, dim), f32),
            pltpu.VMEM((2, full, vb), bf16),
            pltpu.VMEM((NB, 1, vb), f32),
            col, col, col, coli, coli, col, col,
            pltpu.VMEM((8, 2, nc, LANES), f32),
            pltpu.VMEM((nc, 4, 8, LANES), f32),
            pltpu.VMEM((nc, 8, 4, 8, LANES), f32),
            pltpu.VMEM((2, full // 2, dim), f32),
            pltpu.VMEM((2, 2, own, dim), f32),
            pltpu.VMEM((2, own, dim), f32),
            pltpu.VMEM((8, dim), f32),
            pltpu.VMEM((8, 8, dim), f32),
            dma((NB,)), dma((nc, 4)), dma((nc, 7)), dma((nc, 3)), dma((8,)), dma((8,)), dma((nc, 8)), dma((nc, 8)),
            dma((2,)), dma((2,)), dma((2, 2)), dma((2, 2)), dma((2,)), dma((2,)),
            reg, reg, reg, dma((8,)), dma((8,)), dma((2,)), dma((nc,)),
        ],
        compiler_params=pltpu.CompilerParams(collective_id=0, has_side_effects=True, vmem_limit_bytes=67043328),
        cost_estimate=pl.CostEstimate(flops=flops, bytes_accessed=100_000_000, transcendentals=0),
    )(hidden, gamma, beta, embed.reshape(NB, vb, dim), valid, tm)


def grad_kernel(dz_ref, x_ref, o_ref):
    o_ref[...] = lax.dot_general(dz_ref[...], x_ref[...], (((0,), (0,)), ((), ())), preferred_element_type=jnp.float32)


def embed_grad(dz, x):
    nb, toks, vb = dz.shape
    dim = x.shape[1]
    mb = vb // 2
    return pl.pallas_call(
        grad_kernel,
        grid=(nb, 2),
        out_shape=jax.ShapeDtypeStruct((nb * vb, dim), jnp.float32),
        in_specs=[
            pl.BlockSpec((None, toks, mb), lambda i, k: (i, 0, k)),
            pl.BlockSpec((toks, dim), lambda i, k: (0, 0), pipeline_mode=pl.Buffered(1)),
        ],
        out_specs=pl.BlockSpec((mb, dim), lambda i, k: (i * 2 + k, 0)),
        compiler_params=pltpu.CompilerParams(vmem_limit_bytes=62 * 1024 * 1024),
        cost_estimate=pl.CostEstimate(flops=2 * toks * nb * vb * dim, bytes_accessed=100_000_000, transcendentals=0),
    )(dz, x)


def solution(mesh):
    tok_spec = P(("dp", "tp"))
    row_spec = P(("dp", "tp"), None)

    def local_step(hidden, gamma, beta, embed, valid, tgt, mask):
        tok, dim = hidden.shape
        own = tok // 8
        me = lax.axis_index("tp")
        core, xc, yc = me % 2, (me // 2) % 2, me // 4
        slot = core * 4 + yc * 2 + xc
        tm = jnp.stack([tgt, mask]).astype(jnp.float32).reshape(2, 8, 1, own)
        tm = jnp.where((jnp.arange(2) == xc)[None, None, :, None], tm, 0.0).reshape(2, 8, 2 * own)
        dz, x_all, d_hidden, loss, gb = fused(
            hidden, gamma.reshape(1, dim), beta.reshape(1, dim), embed, valid.reshape(NB, 1, -1), tm)
        d_embed = embed_grad(dz, x_all.reshape(-1, dim))
        tok_loss = lax.dynamic_index_in_dim(loss.reshape(8, 8, own), slot, axis=1, keepdims=False).reshape(-1)
        mean_loss = jnp.sum(loss) / gb[2, :1]
        return tok_loss, mean_loss, d_hidden, d_embed, gb[0], gb[1]

    return jax.shard_map(
        local_step,
        mesh=mesh,
        in_specs=(row_spec, P(), P(), P("tp", None), P("tp"), tok_spec, tok_spec),
        out_specs=(tok_spec, P("dp"), row_spec, row_spec, P("dp"), P("dp")),
        check_vma=False,
    )
```

```python
import functools

import jax
import jax.numpy as jnp
from jax import lax
from jax.experimental import pallas as pl
from jax.experimental.pallas import tpu as pltpu
from jax.sharding import PartitionSpec as P

LN_EPS = 1e-5
LANES = 128
NB = 5
AHEAD = 3
LAG = NB + 1
LOW = float(jnp.finfo(jnp.float32).min)
MESH = pl.DeviceIdType.MESH
NT = (((1,), (1,)), ((), ()))


def _spread(row):
    return jnp.broadcast_to(row, (LANES, LANES)).T


def fused_kernel(
    hid_ref, gam_in, bet_in, valid_in, tgt_in, mask_in, emb_hbm,
    dz_hbm, xall_hbm, dh_ref, tl_ref, gb_ref,
    par_ref, tm_src, loss_ref, xv, ev, ring, acc, dzb, bias, m_sc, s_sc, p_sc, t1_sc, t2_sc, lse_sc, w_sc,
    tm_all, st_send, st_recv, r0, r1, r2, gb_send, gb_recv,
    e_sem, ag_send, ag_recv, fw_send, tm_send, tm_recv, st_ssem, st_rsem,
    s0, q0, s1, q1, s2, q2, free0, free1, free2, gb_ssem, gb_rsem, dz_sem, x_sem,
):
    nc, tok, dim = xv.shape
    vb = ev.shape[1]
    own = tok // 8
    half = tok // 2
    me = lax.axis_index("tp")
    core = lax.rem(me, 2)
    xc = lax.rem(me // 2, 2)
    yc = me // 4

    def dev(y, x, k):
        return y * 4 + x * 2 + k

    def slot_of(y, x, k):
        return k * 4 + y * 2 + x

    sib = dev(yc, xc, 1 - core)
    xn = dev(yc, 1 - xc, core)
    yn = dev(1 - yc, xc, core)
    dn = dev(1 - yc, 1 - xc, core)
    remote = ((xn, slot_of(yc, 1 - xc, core)), (yn, slot_of(1 - yc, xc, core)), (dn, slot_of(1 - yc, 1 - xc, core)))
    my_slot = slot_of(yc, xc, core)
    first_n = jnp.where(core == 0, xn, yn)
    second_n = jnp.where(core == 0, yn, xn)

    def rcopy(src, dst, ssem, rsem, to):
        return pltpu.make_async_remote_copy(src_ref=src, dst_ref=dst, send_sem=ssem, recv_sem=rsem, device_id={"tp": to}, device_id_type=MESH)

    def rows(slot):
        return pl.ds(pl.multiple_of(slot * own, own), own)

    for j in range(NB):
        pltpu.make_async_copy(emb_hbm.at[j], ev.at[j], e_sem.at[j]).start()

    barrier = pltpu.get_barrier_semaphore()
    for k in range(1, 8):
        pl.semaphore_signal(barrier, inc=1, device_id={"tp": lax.rem(me + k, 8)}, device_id_type=MESH)
    pl.semaphore_wait(barrier, 7)

    lane1 = lax.broadcasted_iota(jnp.int32, (1, LANES), 1)
    mine = (lane1 >= LANES // 2) == (xc == 1)
    for i, ref in enumerate((tgt_in, mask_in)):
        for c in range(nc):
            row = ref[c // 2:c // 2 + 1].astype(jnp.float32)
            row = jnp.where(xc == c % 2, row, pltpu.roll(row, LANES // 2, 1))
            tm_src[i, c:c + 1] = jnp.where(mine, row, 0.0)
    for r in range(dim // LANES):
        par_ref[0:1, pl.ds(r * LANES, LANES)] = gam_in[r:r + 1]
        par_ref[1:2, pl.ds(r * LANES, LANES)] = bet_in[r:r + 1]
    tm_all[me] = tm_src[...]

    def tm_copy(k):
        return rcopy(tm_src, tm_all.at[me], tm_send.at[k], tm_recv.at[k], lax.rem(me + k, 8))

    for k in range(1, 8):
        tm_copy(k).start()

    def ln(c):
        h = hid_ref[pl.ds(pl.multiple_of(c * own, own), own), :].astype(jnp.float32)
        cen = h - jnp.mean(h, axis=1, keepdims=True)
        rstd = lax.rsqrt(jnp.mean(cen * cen, axis=1, keepdims=True) + LN_EPS)
        return cen * rstd, rstd

    def ag_copy(c, k):
        r = xv.at[c, rows(my_slot)]
        return rcopy(r, r, ag_send.at[c, k], ag_recv.at[c, k], (xn, yn, dn, sib)[k])

    def fw_copy(c, k):
        r = xv.at[c, rows(remote[k][1])]
        return rcopy(r, r, fw_send.at[c, k], ag_recv.at[c, 4 + k], sib)

    def ag_start(c):
        for k in (2, 0, 1, 3):
            ag_copy(c, k).start()

    def ln_body(c, _):
        xhat, _r = ln(c)
        xv[c, rows(my_slot), :] = (xhat * par_ref[0:1] + par_ref[1:2]).astype(jnp.bfloat16)

        @pl.when((c >= 1) & (c <= AHEAD))
        def _():
            ag_start(c - 1)
        return 0

    lax.fori_loop(0, nc, ln_body, 0)

    for r in range(NB * vb // LANES):
        col = pl.ds(r % (vb // LANES) * LANES, LANES)
        bias[r // (vb // LANES), :, col] = jnp.where(valid_in[r:r + 1] > 0, 0.0, -jnp.inf)
    gb_send[...] = jnp.zeros_like(gb_send)

    def recv_remote(c):
        for k in range(3):
            ag_copy(c, k).wait_recv()

    def forward(c):
        recv_remote(c)
        for k in range(3):
            fw_copy(c, k).start()

    for k in range(1, 8):
        tm_copy(k).wait_recv()
    count = jnp.zeros((8, LANES), jnp.float32)
    for d in range(8):
        count = count + tm_all[d, 1]
    count = jnp.sum(jnp.sum(count, axis=1, keepdims=True), axis=0, keepdims=True)
    inv_n = 1.0 / count

    def tm_rows(c, which):
        out = []
        for q in range(4):
            k, y = q // 2, q % 2
            out.append(tm_all[dev(y, 0, k), which, pl.ds(c, 1), :] + tm_all[dev(y, 1, k), which, pl.ds(c, 1), :])
        return out

    forward(0)
    lane = lax.broadcasted_iota(jnp.int32, (tok, LANES), 1)

    def st_copy(c, k):
        return rcopy(st_send.at[c], st_recv.at[c, me], st_ssem.at[c, k], st_rsem.at[c, k], lax.rem(me + k, 8))

    def send_stats(c):
        li = lax.broadcasted_iota(jnp.int32, (LANES, LANES), 1)
        for q in range(4):
            r = pl.ds(q * LANES, LANES)
            m = m_sc[r]
            mx = jnp.max(m, axis=1, keepdims=True)
            s = jnp.sum(s_sc[r] * jnp.exp(m - mx), axis=1, keepdims=True)
            p = jnp.sum(p_sc[r], axis=1, keepdims=True)
            v = jnp.where(li == 0, mx, jnp.where(li == 1, s, p))
            st_send[c, q] = v.T[:8]
        st_recv[c, me] = st_send[c]
        for k in range(1, 8):
            st_copy(c, k).start()

    def use_stats(c):
        for k in range(1, 8):
            st_copy(c, k).wait_recv()
        tg = tm_rows(c, 0)
        mk = tm_rows(c, 1)
        for q in range(4):
            mx = st_recv[c, 0, q, 0:1]
            for d in range(1, 8):
                mx = jnp.maximum(mx, st_recv[c, d, q, 0:1])
            s = jnp.zeros_like(mx)
            p = jnp.zeros_like(mx)
            for d in range(8):
                s = s + st_recv[c, d, q, 1:2] * jnp.exp(st_recv[c, d, q, 0:1] - mx)
                p = p + st_recv[c, d, q, 2:3]
            lse = mx + jnp.log(s)
            loss_ref[c, pl.ds(q, 1), :] = (lse - p) * mk[q]
            w = mk[q] * inv_n
            r = pl.ds(q * LANES, LANES)
            lse_sc[r] = _spread(lse - jnp.log(w))
            w_sc[r] = _spread(w)
            t2_sc[r] = _spread(tg[q]).astype(jnp.int32)

    def begin_chunk(c):
        for k in range(3, 7):
            if k == 3:
                ag_copy(c, 3).wait_recv()
            else:
                fw_copy(c, k - 4).wait_recv()
        pltpu.make_async_copy(xv.at[c], xall_hbm.at[c], x_sem.at[c]).start()
        for n in range(2):
            @pl.when((c >= 1) & (AHEAD + 2 * (c - 1) + n < nc))
            def _(n=n):
                ag_start(AHEAD + 2 * (c - 1) + n)
        m_sc[...] = jnp.full(m_sc.shape, LOW, jnp.float32)
        s_sc[...] = jnp.zeros_like(s_sc)
        p_sc[...] = jnp.zeros_like(p_sc)
        tg = tm_rows(c, 0)
        for q in range(4):
            t1_sc[pl.ds(q * LANES, LANES)] = _spread(tg[q]).astype(jnp.int32)

    def first_src(b):
        return jnp.where(core == 0, b * 2 + (1 - xc), (1 - yc) * 2 + b)

    def first_keep(b):
        return jnp.where(core == 0, b * 2 + xc, yc * 2 + b)

    own2 = jnp.where(core == 0, yc, xc)

    def c0(c):
        a = lax.rem(c, 2)
        return rcopy(acc.at[a, pl.ds(pl.multiple_of((1 - core) * half, half), half)], r0.at[a], s0.at[a], q0.at[a], sib)

    def c1(c, b):
        a = lax.rem(c, 2)
        return rcopy(r0.at[a, rows(first_src(b))], r1.at[a, b], s1.at[a, b], q1.at[a, b], first_n)

    def c2(c):
        a = lax.rem(c, 2)
        return rcopy(r1.at[a, 1 - own2], r2.at[a], s2.at[a], q2.at[a], second_n)

    def stage0(c):
        @pl.when(c >= 2)
        def _():
            pl.semaphore_wait(free0, 1)
        c0(c).start()

    def stage1(c):
        a = lax.rem(c, 2)
        c0(c).wait()
        r0[a] = r0[a] + acc[a, pl.ds(pl.multiple_of(core * half, half), half)]

        @pl.when(c >= 2)
        def _():
            pl.semaphore_wait(free1, 1)
        for b in range(2):
            c1(c, b).start()

    def stage2(c):
        a = lax.rem(c, 2)
        for b in range(2):
            c1(c, b).wait()
        for b in range(2):
            r1[a, b] = r1[a, b] + r0[a, rows(first_keep(b))]

        @pl.when(c >= 2)
        def _():
            pl.semaphore_wait(free2, 1)
        c2(c).start()

        @pl.when(c < nc - 2)
        def _():
            pl.semaphore_signal(free0, inc=1, device_id={"tp": sib}, device_id_type=MESH)

    def stage3(c):
        a = lax.rem(c, 2)
        c2(c).wait()
        dy = r1[a, own2] + r2[a]

        @pl.when(c < nc - 2)
        def _():
            pl.semaphore_signal(free1, inc=1, device_id={"tp": first_n}, device_id_type=MESH)
            pl.semaphore_signal(free2, inc=1, device_id={"tp": second_n}, device_id_type=MESH)
        xhat, rstd = ln(c)
        gb_send[0:1] += jnp.sum(dy * xhat, axis=0, keepdims=True)
        gb_send[1:2] += jnp.sum(dy, axis=0, keepdims=True)
        dxh = dy * par_ref[0:1]
        m1 = jnp.mean(dxh, axis=1, keepdims=True)
        m2 = jnp.mean(dxh * xhat, axis=1, keepdims=True)
        dh_ref[pl.ds(pl.multiple_of(c * own, own), own), :] = (rstd * (dxh - m1 - xhat * m2)).astype(jnp.bfloat16)

    base = me * (NB * vb)

    def dz_copy(t):
        a = lax.rem(t, 2)
        t2 = t - LAG
        return pltpu.make_async_copy(dzb.at[a], dz_hbm.at[lax.rem(t2, NB), pl.ds(pl.multiple_of((t2 // NB) * tok, tok), tok)], dz_sem.at[a])

    def compute(t, do1, do2):
        slot = lax.rem(t, LAG)
        a2 = lax.rem(t, 2)
        cut = (vb // LANES + 1) // 4 * 2 * LANES if vb % 256 else (vb // 256 + 1) // 2 * 256
        pieces = ((0, cut), (cut, vb))
        j1 = lax.rem(t, NB)
        zs = []
        if do2:
            t2 = t - LAG
            j2 = lax.rem(t2, NB)
            a = lax.rem(t2 // NB, 2)
            tr2 = t2_sc[...] - (base + j2 * vb)
        for lo, hi in pieces:
            if do2:
                for col in range(lo, hi, LANES):
                    p = jnp.exp(ring[slot, :, pl.ds(col, LANES)] - lse_sc[...])
                    p = p - jnp.where(tr2 == lane + col, w_sc[...], 0.0)
                    dzb[a2, :, pl.ds(col, LANES)] = p.astype(jnp.bfloat16)
            if do1:
                zs.append(lax.dot_general(xv[t // NB], ev[j1, pl.ds(lo, hi - lo), :], NT, preferred_element_type=jnp.float32))
        if do1:
            tr1 = t1_sc[...] - (base + j1 * vb)
        for n, (lo, hi) in enumerate(pieces):
            w = pl.ds(lo, hi - lo)
            if do2:
                acc[a, :, pl.ds(lo * dim // vb, (hi - lo) * dim // vb)] += jnp.dot(
                    dzb[a2], ev[j2, :, pl.ds(lo * dim // vb, (hi - lo) * dim // vb)], preferred_element_type=jnp.float32)
            if do1:
                z = zs[n] + bias[j1, :, w]
                ring[slot, :, w] = z
                cols = [z[:, k * LANES:(k + 1) * LANES] for k in range((hi - lo) // LANES)]
                m0 = m_sc[...]
                m = m0
                for q in cols:
                    m = jnp.maximum(m, q)
                s = s_sc[...] * jnp.exp(m0 - m)
                pk = p_sc[...]
                for k, q in enumerate(cols):
                    s = s + jnp.exp(q - m)
                    pk = pk + jnp.where(tr1 == lane + (lo + k * LANES), q, 0.0)
                m_sc[...] = m
                s_sc[...] = s
                p_sc[...] = pk

    def step(t, do1, do2):
        ph = lax.rem(t, NB)
        if do1:
            @pl.when(ph == 0)
            def _():
                begin_chunk(t // NB)

            @pl.when((ph == 2) & (t // NB + 1 < nc))
            def _():
                forward(t // NB + 1)

            @pl.when(t < NB)
            def _():
                pltpu.make_async_copy(emb_hbm.at[ph], ev.at[ph], e_sem.at[ph]).wait()
        if do2:
            @pl.when((ph == 1) & (t >= 11))
            def _():
                stage0((t - 11) // NB)

            @pl.when(ph == 1)
            def _():
                c = (t - LAG) // NB
                use_stats(c)
                acc[lax.rem(c, 2)] = jnp.zeros((tok, dim), jnp.float32)

            @pl.when((ph == 2) & (t >= 17))
            def _():
                stage3((t - 17) // NB)

            @pl.when((ph == 2) & (t >= 12))
            def _():
                stage1((t - 12) // NB)

            @pl.when((ph == 0) & (t >= 15))
            def _():
                stage2((t - 15) // NB)

            @pl.when(t >= LAG + 2)
            def _():
                dz_copy(t - 2).wait()
        compute(t, do1, do2)
        if do2:
            dz_copy(t).start()
        if do1:
            @pl.when(ph == NB - 1)
            def _():
                send_stats(t // NB)

    def loop(lo, hi, do1, do2):
        def body(t, _):
            step(t, do1, do2)
            return 0
        lax.fori_loop(lo, hi, body, 0)

    total = NB * nc
    loop(0, LAG, True, False)
    loop(LAG, total, True, True)
    loop(total, total + LAG, False, True)

    last = nc - 1
    stage0(last)
    stage3(last - 1)
    stage1(last)
    stage2(last)
    stage3(last)

    def gb_copy(k):
        return rcopy(gb_send, gb_recv.at[me], gb_ssem.at[k], gb_rsem.at[k], lax.rem(me + k, 8))

    for k in range(1, 8):
        gb_copy(k).start()
    gb_recv[me] = gb_send[...]
    for t in (total + LAG - 2, total + LAG - 1):
        dz_copy(t).wait()

    def drain(c, _):
        for k in range(4):
            ag_copy(c, k).wait_send()
        for k in range(3):
            fw_copy(c, k).wait_send()
        for k in range(1, 8):
            st_copy(c, k).wait_send()
        pltpu.make_async_copy(xv.at[c], xall_hbm.at[c], x_sem.at[c]).wait()
        return 0

    lax.fori_loop(0, nc, drain, 0)
    for k in range(1, 8):
        tm_copy(k).wait_send()
        gb_copy(k).wait()
    tot = gb_recv[0]
    for d in range(1, 8):
        tot = tot + gb_recv[d]
    gb_ref[...] = tot
    mean = jnp.zeros((4, LANES), jnp.float32)
    for c in range(nc):
        mean = mean + loss_ref[c]
    mean = jnp.sum(jnp.sum(mean, axis=1, keepdims=True), axis=0, keepdims=True) / count
    gb_ref[2:3] = jnp.broadcast_to(mean, (1, dim))
    for r in range(nc // 2):
        halves = []
        for n in range(2):
            row = loss_ref[2 * r + n, pl.ds(my_slot // 2, 1), :]
            halves.append(jnp.where(xc == n, row, pltpu.roll(row, LANES // 2, 1)))
        tl_ref[r:r + 1] = jnp.where(lane1 < LANES // 2, halves[0], halves[1])


def fused(hidden, gamma, beta, valid, tgt, mask, embed):
    tok, dim = hidden.shape
    nc = 8
    own = tok // nc
    vb = embed.shape[0] // NB
    full = own * 8
    f32, bf16 = jnp.float32, jnp.bfloat16
    sds = jax.ShapeDtypeStruct
    vmem = pl.BlockSpec(memory_space=pltpu.VMEM)
    hbm = pl.BlockSpec(memory_space=pl.ANY)
    col = pltpu.VMEM((full, LANES), f32)
    coli = pltpu.VMEM((full, LANES), jnp.int32)
    dma, reg = pltpu.SemaphoreType.DMA, pltpu.SemaphoreType.REGULAR
    flops = 4 * full * nc * embed.shape[0] * dim
    return pl.pallas_call(
        fused_kernel,
        out_shape=(
            sds((NB, nc * full, vb), bf16),
            sds((nc, full, dim), bf16),
            sds((tok, dim), bf16),
            sds((nc // 2, LANES), f32),
            sds((8, dim), f32),
        ),
        in_specs=[vmem] * 6 + [hbm],
        out_specs=(hbm, hbm, vmem, vmem, vmem),
        scratch_shapes=[
            pltpu.VMEM((8, dim), f32),
            pltpu.VMEM((2, nc, LANES), f32),
            pltpu.VMEM((nc, 4, LANES), f32),
            pltpu.VMEM((nc, full, dim), bf16),
            pltpu.VMEM((NB, vb, dim), bf16),
            pltpu.VMEM((LAG, full, vb), f32),
            pltpu.VMEM((2, full, dim), f32),
            pltpu.VMEM((2, full, vb), bf16),
            pltpu.VMEM((NB, 1, vb), f32),
            col, col, col, coli, coli, col, col,
            pltpu.VMEM((8, 2, nc, LANES), f32),
            pltpu.VMEM((nc, 4, 8, LANES), f32),
            pltpu.VMEM((nc, 8, 4, 8, LANES), f32),
            pltpu.VMEM((2, full // 2, dim), f32),
            pltpu.VMEM((2, 2, own, dim), f32),
            pltpu.VMEM((2, own, dim), f32),
            pltpu.VMEM((8, dim), f32),
            pltpu.VMEM((8, 8, dim), f32),
            dma((NB,)), dma((nc, 4)), dma((nc, 7)), dma((nc, 3)), dma((8,)), dma((8,)), dma((nc, 8)), dma((nc, 8)),
            dma((2,)), dma((2,)), dma((2, 2)), dma((2, 2)), dma((2,)), dma((2,)),
            reg, reg, reg, dma((8,)), dma((8,)), dma((2,)), dma((nc,)),
        ],
        compiler_params=pltpu.CompilerParams(collective_id=0, has_side_effects=True, vmem_limit_bytes=67043328),
        cost_estimate=pl.CostEstimate(flops=flops, bytes_accessed=100_000_000, transcendentals=0),
    )(hidden, gamma, beta, valid, tgt, mask, embed.reshape(NB, vb, dim))


def grad_kernel(dz_ref, x_ref, dh_in, tl_in, gb_in, o_ref, dh_ref, tl_ref, dg_ref, db_ref, ml_ref):
    @pl.when((pl.program_id(0) == 0) & (pl.program_id(1) == 0))
    def _():
        dh_ref[...] = dh_in[...]
        tl_ref[...] = tl_in[...]
        for r in range(dg_ref.shape[0]):
            dg_ref[r:r + 1] = gb_in[0:1, r * LANES:(r + 1) * LANES]
            db_ref[r:r + 1] = gb_in[1:2, r * LANES:(r + 1) * LANES]
        ml_ref[...] = gb_in[2:3, 0:1]

    o_ref[...] = lax.dot_general(dz_ref[...], x_ref[...], (((0,), (0,)), ((), ())), preferred_element_type=jnp.float32)


def embed_grad(dz, x, d_hidden, tl, gb):
    nb, toks, vb = dz.shape
    dim = x.shape[1]
    mb = vb // 2
    f32 = jnp.float32
    sds = jax.ShapeDtypeStruct

    def whole(shape):
        return pl.BlockSpec(shape, lambda i, k: (0, 0), pipeline_mode=pl.Buffered(1))

    return pl.pallas_call(
        grad_kernel,
        grid=(nb, 2),
        out_shape=(
            sds((nb * vb, dim), f32), sds(d_hidden.shape, d_hidden.dtype), sds(tl.shape, f32),
            sds((dim // LANES, LANES), f32), sds((dim // LANES, LANES), f32), sds((1, 1), f32),
        ),
        in_specs=[
            pl.BlockSpec((None, toks, mb), lambda i, k: (i, 0, k)),
            whole((toks, dim)), whole(d_hidden.shape), whole(tl.shape), whole(gb.shape),
        ],
        out_specs=(
            pl.BlockSpec((mb, dim), lambda i, k: (i * 2 + k, 0)),
            whole(d_hidden.shape), whole(tl.shape), whole((dim // LANES, LANES)), whole((dim // LANES, LANES)), whole((1, 1)),
        ),
        compiler_params=pltpu.CompilerParams(vmem_limit_bytes=62 * 1024 * 1024),
        cost_estimate=pl.CostEstimate(flops=2 * toks * nb * vb * dim, bytes_accessed=100_000_000, transcendentals=0),
    )(dz, x, d_hidden, tl, gb)


def solution(mesh):
    tok_spec = P(("dp", "tp"))
    row_spec = P(("dp", "tp"), None)

    def local_step(hidden, gamma, beta, embed, valid, tgt, mask):
        tok, dim = hidden.shape
        def rows(v):
            return v.reshape(-1, LANES)

        dz, x_all, d_hidden, tl, gb = fused(hidden, rows(gamma), rows(beta), rows(valid), rows(tgt), rows(mask), embed)
        d_embed, d_hidden, tl, dg, db, ml = embed_grad(dz, x_all.reshape(-1, dim), d_hidden, tl, gb)
        return tl.reshape(-1), ml.reshape(1), d_hidden, d_embed, dg.reshape(-1), db.reshape(-1)

    return jax.shard_map(
        local_step,
        mesh=mesh,
        in_specs=(row_spec, P(), P(), P("tp", None), P("tp"), tok_spec, tok_spec),
        out_specs=(tok_spec, P("dp"), row_spec, row_spec, P("dp"), P("dp")),
        check_vma=False,
    )
```

```python
import functools

import jax
import jax.numpy as jnp
from jax import lax
from jax.experimental import pallas as pl
from jax.experimental.pallas import tpu as pltpu
from jax.sharding import PartitionSpec as P

LN_EPS = 1e-5
LANES = 128
NB = 5
AHEAD = 3
LAG = NB + 1
LOW = float(jnp.finfo(jnp.float32).min)
MESH = pl.DeviceIdType.MESH
NT = (((1,), (1,)), ((), ()))


def _spread(row):
    return jnp.broadcast_to(row, (LANES, LANES)).T


def fused_kernel(
    hid_ref, gam_in, bet_in, valid_in, tgt_in, mask_in, emb_hbm,
    dz_hbm, xall_hbm, de_hbm, dh_ref, tl_ref, gb_ref,
    par_ref, tm_src, loss_ref, xv, ev, ring, acc, dzb, bias, m_sc, s_sc, p_sc, t1_sc, t2_sc, lse_sc, w_sc,
    tm_all, st_send, st_recv, r0, r1, r2, gb_send, gb_recv,
    e_sem, ag_send, ag_recv, fw_send, tm_send, tm_recv, st_ssem, st_rsem,
    s0, q0, s1, q1, s2, q2, free0, free1, free2, gb_ssem, gb_rsem, dz_sem, x_sem, fz_sem, de_sem,
):
    nc, tok, dim = xv.shape
    vb = ev.shape[1]
    own = tok // 8
    half = tok // 2
    me = lax.axis_index("tp")
    core = lax.rem(me, 2)
    xc = lax.rem(me // 2, 2)
    yc = me // 4

    def dev(y, x, k):
        return y * 4 + x * 2 + k

    def slot_of(y, x, k):
        return k * 4 + y * 2 + x

    sib = dev(yc, xc, 1 - core)
    xn = dev(yc, 1 - xc, core)
    yn = dev(1 - yc, xc, core)
    dn = dev(1 - yc, 1 - xc, core)
    remote = ((xn, slot_of(yc, 1 - xc, core)), (yn, slot_of(1 - yc, xc, core)), (dn, slot_of(1 - yc, 1 - xc, core)))
    my_slot = slot_of(yc, xc, core)
    first_n = jnp.where(core == 0, xn, yn)
    second_n = jnp.where(core == 0, yn, xn)

    def rcopy(src, dst, ssem, rsem, to):
        return pltpu.make_async_remote_copy(src_ref=src, dst_ref=dst, send_sem=ssem, recv_sem=rsem, device_id={"tp": to}, device_id_type=MESH)

    def rows(slot):
        return pl.ds(pl.multiple_of(slot * own, own), own)

    for j in range(NB):
        pltpu.make_async_copy(emb_hbm.at[j], ev.at[j], e_sem.at[j]).start()

    barrier = pltpu.get_barrier_semaphore()
    for k in range(1, 8):
        pl.semaphore_signal(barrier, inc=1, device_id={"tp": lax.rem(me + k, 8)}, device_id_type=MESH)

    lane1 = lax.broadcasted_iota(jnp.int32, (1, LANES), 1)
    mine = (lane1 >= LANES // 2) == (xc == 1)
    for i, ref in enumerate((tgt_in, mask_in)):
        for c in range(nc):
            row = ref[c // 2:c // 2 + 1].astype(jnp.float32)
            row = jnp.where(xc == c % 2, row, pltpu.roll(row, LANES // 2, 1))
            tm_src[i, c:c + 1] = jnp.where(mine, row, 0.0)
    for r in range(dim // LANES):
        par_ref[0:1, pl.ds(r * LANES, LANES)] = gam_in[r:r + 1]
        par_ref[1:2, pl.ds(r * LANES, LANES)] = bet_in[r:r + 1]
    tm_all[me] = tm_src[...]

    def tm_copy(k):
        return rcopy(tm_src, tm_all.at[me], tm_send.at[k], tm_recv.at[k], lax.rem(me + k, 8))

    def ln(c):
        h = hid_ref[pl.ds(pl.multiple_of(c * own, own), own), :].astype(jnp.float32)
        cen = h - jnp.mean(h, axis=1, keepdims=True)
        rstd = lax.rsqrt(jnp.mean(cen * cen, axis=1, keepdims=True) + LN_EPS)
        return cen * rstd, rstd

    def ag_copy(c, k):
        r = xv.at[c, rows(my_slot)]
        return rcopy(r, r, ag_send.at[c, k], ag_recv.at[c, k], (xn, yn, dn, sib)[k])

    def fw_copy(c, k):
        r = xv.at[c, rows(remote[k][1])]
        return rcopy(r, r, fw_send.at[c, k], ag_recv.at[c, 4 + k], sib)

    def ag_start(c):
        for k in (2, 0, 1, 3):
            ag_copy(c, k).start()

    def ln_store(c):
        xhat, _ = ln(c)
        xv[c, rows(my_slot), :] = (xhat * par_ref[0:1] + par_ref[1:2]).astype(jnp.bfloat16)

    for c in range(2):
        ln_store(c)
    pl.semaphore_wait(barrier, 7)
    ag_start(0)
    for k in range(1, 8):
        tm_copy(k).start()

    def ln_body(c, _):
        ln_store(c)

        @pl.when(c <= AHEAD)
        def _():
            ag_start(c - 1)
        return 0

    lax.fori_loop(2, nc, ln_body, 0)
    for r in range(NB * vb // LANES):
        col = pl.ds(r % (vb // LANES) * LANES, LANES)
        bias[r // (vb // LANES), :, col] = jnp.where(valid_in[r:r + 1] > 0, 0.0, -jnp.inf)
    gb_send[...] = jnp.zeros_like(gb_send)

    def recv_remote(c):
        for k in range(3):
            ag_copy(c, k).wait_recv()

    def forward(c):
        recv_remote(c)
        for k in range(3):
            fw_copy(c, k).start()

    for k in range(1, 8):
        tm_copy(k).wait_recv()
    count = jnp.zeros((8, LANES), jnp.float32)
    for d in range(8):
        count = count + tm_all[d, 1]
    count = jnp.sum(jnp.sum(count, axis=1, keepdims=True), axis=0, keepdims=True)
    inv_n = 1.0 / count

    def tm_rows(c, which):
        out = []
        for q in range(4):
            k, y = q // 2, q % 2
            out.append(tm_all[dev(y, 0, k), which, pl.ds(c, 1), :] + tm_all[dev(y, 1, k), which, pl.ds(c, 1), :])
        return out

    forward(0)
    lane = lax.broadcasted_iota(jnp.int32, (tok, LANES), 1)

    def st_copy(c, k):
        return rcopy(st_send.at[c], st_recv.at[c, me], st_ssem.at[c, k], st_rsem.at[c, k], lax.rem(me + k, 8))

    def send_stats(c):
        for q in range(4):
            r = pl.ds(q * LANES, LANES)
            m = m_sc[r].T
            mx = jnp.max(m, axis=0, keepdims=True)
            st_send[c, q, 0:1] = mx
            st_send[c, q, 1:2] = jnp.sum(s_sc[r].T * jnp.exp(m - mx), axis=0, keepdims=True)
            st_send[c, q, 2:3] = jnp.sum(p_sc[r].T, axis=0, keepdims=True)
        st_recv[c, me] = st_send[c]
        for k in range(1, 8):
            st_copy(c, k).start()

    def use_stats(c):
        for k in range(1, 8):
            st_copy(c, k).wait_recv()
        tg = tm_rows(c, 0)
        mk = tm_rows(c, 1)
        for q in range(4):
            mx = st_recv[c, 0, q, 0:1]
            for d in range(1, 8):
                mx = jnp.maximum(mx, st_recv[c, d, q, 0:1])
            s = jnp.zeros_like(mx)
            p = jnp.zeros_like(mx)
            for d in range(8):
                s = s + st_recv[c, d, q, 1:2] * jnp.exp(st_recv[c, d, q, 0:1] - mx)
                p = p + st_recv[c, d, q, 2:3]
            lse = mx + jnp.log(s)
            loss_ref[c, pl.ds(q, 1), :] = (lse - p) * mk[q]
            w = mk[q] * inv_n
            r = pl.ds(q * LANES, LANES)
            lse_sc[r] = _spread(lse - jnp.log(w))
            w_sc[r] = _spread(w)
            t2_sc[r] = _spread(tg[q]).astype(jnp.int32)

    def begin_chunk(c):
        for k in range(3, 7):
            if k == 3:
                ag_copy(c, 3).wait_recv()
            else:
                fw_copy(c, k - 4).wait_recv()
        pltpu.make_async_copy(xv.at[c], xall_hbm.at[c], x_sem.at[c]).start()
        for n in range(2):
            @pl.when((c >= 1) & (AHEAD + 2 * (c - 1) + n < nc))
            def _(n=n):
                ag_start(AHEAD + 2 * (c - 1) + n)
        m_sc[...] = jnp.full(m_sc.shape, LOW, jnp.float32)
        s_sc[...] = jnp.zeros_like(s_sc)
        p_sc[...] = jnp.zeros_like(p_sc)
        tg = tm_rows(c, 0)
        for q in range(4):
            t1_sc[pl.ds(q * LANES, LANES)] = _spread(tg[q]).astype(jnp.int32)

    def first_src(b):
        return jnp.where(core == 0, b * 2 + (1 - xc), (1 - yc) * 2 + b)

    def first_keep(b):
        return jnp.where(core == 0, b * 2 + xc, yc * 2 + b)

    own2 = jnp.where(core == 0, yc, xc)

    def c0(c):
        a = lax.rem(c, 2)
        return rcopy(acc.at[a, pl.ds(pl.multiple_of((1 - core) * half, half), half)], r0.at[a], s0.at[a], q0.at[a], sib)

    def c1(c, b):
        a = lax.rem(c, 2)
        return rcopy(r0.at[a, rows(first_src(b))], r1.at[a, b], s1.at[a, b], q1.at[a, b], first_n)

    def c2(c):
        a = lax.rem(c, 2)
        return rcopy(r1.at[a, 1 - own2], r2.at[a], s2.at[a], q2.at[a], second_n)

    def stage0(c):
        @pl.when(c >= 2)
        def _():
            pl.semaphore_wait(free0, 1)
        c0(c).start()

    def stage1(c):
        a = lax.rem(c, 2)
        c0(c).wait()
        r0[a] = r0[a] + acc[a, pl.ds(pl.multiple_of(core * half, half), half)]

        @pl.when(c >= 2)
        def _():
            pl.semaphore_wait(free1, 1)
        for b in range(2):
            c1(c, b).start()

    def stage2(c):
        a = lax.rem(c, 2)
        for b in range(2):
            c1(c, b).wait()
        for b in range(2):
            r1[a, b] = r1[a, b] + r0[a, rows(first_keep(b))]

        @pl.when(c >= 2)
        def _():
            pl.semaphore_wait(free2, 1)
        c2(c).start()

        @pl.when(c < nc - 2)
        def _():
            pl.semaphore_signal(free0, inc=1, device_id={"tp": sib}, device_id_type=MESH)

    def stage3(c):
        a = lax.rem(c, 2)
        c2(c).wait()
        dy = r1[a, own2] + r2[a]

        @pl.when(c < nc - 2)
        def _():
            pl.semaphore_signal(free1, inc=1, device_id={"tp": first_n}, device_id_type=MESH)
            pl.semaphore_signal(free2, inc=1, device_id={"tp": second_n}, device_id_type=MESH)
        xhat, rstd = ln(c)
        gb_send[0:1] += jnp.sum(dy * xhat, axis=0, keepdims=True)
        gb_send[1:2] += jnp.sum(dy, axis=0, keepdims=True)
        dxh = dy * par_ref[0:1]
        m1 = jnp.mean(dxh, axis=1, keepdims=True)
        m2 = jnp.mean(dxh * xhat, axis=1, keepdims=True)
        dh_ref[pl.ds(pl.multiple_of(c * own, own), own), :] = (rstd * (dxh - m1 - xhat * m2)).astype(jnp.bfloat16)

    base = me * (NB * vb)

    def dz_copy(t):
        a = lax.rem(t, 2)
        t2 = t - LAG
        return pltpu.make_async_copy(dzb.at[a], dz_hbm.at[lax.rem(t2, NB), pl.ds(pl.multiple_of((t2 // NB) * tok, tok), tok)], dz_sem.at[a])

    def compute(t, do1, do2):
        slot = lax.rem(t, LAG)
        a2 = lax.rem(t, 2)
        cut = (vb // LANES + 1) // 4 * 2 * LANES if vb % 256 else (vb // 256 + 1) // 2 * 256
        pieces = ((0, cut), (cut, vb))
        j1 = lax.rem(t, NB)
        zs = []
        if do2:
            t2 = t - LAG
            j2 = lax.rem(t2, NB)
            a = lax.rem(t2 // NB, 2)
            tr2 = t2_sc[...] - (base + j2 * vb)
        for lo, hi in pieces:
            if do2:
                for col in range(lo, hi, LANES):
                    p = jnp.exp(ring[slot, :, pl.ds(col, LANES)] - lse_sc[...])
                    p = p - jnp.where(tr2 == lane + col, w_sc[...], 0.0)
                    dzb[a2, :, pl.ds(col, LANES)] = p.astype(jnp.bfloat16)
            if do1:
                zs.append(lax.dot_general(xv[t // NB], ev[j1, pl.ds(lo, hi - lo), :], NT, preferred_element_type=jnp.float32))
        if do1:
            tr1 = t1_sc[...] - (base + j1 * vb)
        for n, (lo, hi) in enumerate(pieces):
            w = pl.ds(lo, hi - lo)
            if do2:
                acc[a, :, pl.ds(lo * dim // vb, (hi - lo) * dim // vb)] += jnp.dot(
                    dzb[a2], ev[j2, :, pl.ds(lo * dim // vb, (hi - lo) * dim // vb)], preferred_element_type=jnp.float32)
            if do1:
                z = zs[n] + bias[j1, :, w]
                ring[slot, :, w] = z
                cols = [z[:, k * LANES:(k + 1) * LANES] for k in range((hi - lo) // LANES)]
                m0 = m_sc[...]
                m = m0
                for q in cols:
                    m = jnp.maximum(m, q)
                s = s_sc[...] * jnp.exp(m0 - m)
                pk = p_sc[...]
                for k, q in enumerate(cols):
                    s = s + jnp.exp(q - m)
                    pk = pk + jnp.where(tr1 == lane + (lo + k * LANES), q, 0.0)
                m_sc[...] = m
                s_sc[...] = s
                p_sc[...] = pk

    def step(t, do1, do2):
        ph = lax.rem(t, NB)
        if do1:
            @pl.when(ph == 0)
            def _():
                begin_chunk(t // NB)

            @pl.when((ph == 2) & (t // NB + 1 < nc))
            def _():
                forward(t // NB + 1)

            @pl.when(t < NB)
            def _():
                pltpu.make_async_copy(emb_hbm.at[ph], ev.at[ph], e_sem.at[ph]).wait()
        if do2:
            @pl.when((ph == 1) & (t >= 11))
            def _():
                stage0((t - 11) // NB)

            @pl.when(ph == 1)
            def _():
                c = (t - LAG) // NB
                use_stats(c)
                acc[lax.rem(c, 2)] = jnp.zeros((tok, dim), jnp.float32)

            @pl.when((ph == 2) & (t >= 17))
            def _():
                stage3((t - 17) // NB)

            @pl.when((ph == 2) & (t >= 12))
            def _():
                stage1((t - 12) // NB)

            @pl.when((ph == 0) & (t >= 15))
            def _():
                stage2((t - 15) // NB)

            @pl.when(t >= LAG + 2)
            def _():
                dz_copy(t - 2).wait()
        compute(t, do1, do2)
        if do2:
            dz_copy(t).start()
        if do1:
            @pl.when(ph == NB - 1)
            def _():
                send_stats(t // NB)

    def loop(lo, hi, do1, do2):
        def body(t, _):
            step(t, do1, do2)
            return 0
        lax.fori_loop(lo, hi, body, 0)

    spans = [(n, lo, min(tok, vb - lo)) for n, lo in enumerate(range(0, vb, tok))]

    def fz_copy(c):
        a = lax.rem(c, 2)
        return pltpu.make_async_copy(dz_hbm.at[0, pl.ds(pl.multiple_of(c * tok, tok), tok)], dzb.at[a], fz_sem.at[a])

    def de_copy(n, lo, size):
        return pltpu.make_async_copy(ring.at[n, pl.ds(0, size)], de_hbm.at[pl.ds(lo, size)], de_sem.at[n])

    last = nc - 1

    def fill(f, _):
        @pl.when(f == 0)
        def _():
            stage0(last)
            for n, lo, size in spans:
                ring[n, :size] = jnp.zeros((size, dim), jnp.float32)

        @pl.when(f == 1)
        def _():
            stage3(last - 1)

        @pl.when(f == 2)
        def _():
            stage1(last)

        @pl.when(f == nc - 2)
        def _():
            stage2(last)
        fz_copy(f).wait()
        a = lax.rem(f, 2)
        for n, lo, size in spans:
            ring[n, :size] += lax.dot_general(dzb[a, :, pl.ds(lo, size)], xv[f], (((0,), (0,)), ((), ())), preferred_element_type=jnp.float32)

        @pl.when(f + 2 < nc)
        def _():
            fz_copy(f + 2).start()
        return 0

    total = NB * nc
    loop(0, LAG, True, False)
    loop(LAG, total, True, True)
    loop(total, total + LAG, False, True)
    for c in range(2):
        dz_copy(total + LAG - 2 + c).wait()
        fz_copy(lax.rem(total + LAG + c, 2)).start()
    lax.fori_loop(0, nc, fill, 0)
    for span in spans:
        de_copy(*span).start()
    stage3(last)

    def gb_copy(k):
        return rcopy(gb_send, gb_recv.at[me], gb_ssem.at[k], gb_rsem.at[k], lax.rem(me + k, 8))

    for k in range(1, 8):
        gb_copy(k).start()
    gb_recv[me] = gb_send[...]
    for span in spans:
        de_copy(*span).wait()

    def drain(c, _):
        for k in range(4):
            ag_copy(c, k).wait_send()
        for k in range(3):
            fw_copy(c, k).wait_send()
        for k in range(1, 8):
            st_copy(c, k).wait_send()
        pltpu.make_async_copy(xv.at[c], xall_hbm.at[c], x_sem.at[c]).wait()
        return 0

    lax.fori_loop(0, nc, drain, 0)
    for k in range(1, 8):
        tm_copy(k).wait_send()
        gb_copy(k).wait()
    tot = gb_recv[0]
    for d in range(1, 8):
        tot = tot + gb_recv[d]
    gb_ref[...] = tot
    mean = jnp.zeros((4, LANES), jnp.float32)
    for c in range(nc):
        mean = mean + loss_ref[c]
    mean = jnp.sum(jnp.sum(mean, axis=1, keepdims=True), axis=0, keepdims=True) / count
    gb_ref[2:3] = jnp.broadcast_to(mean, (1, dim))
    for r in range(nc // 2):
        halves = []
        for n in range(2):
            row = loss_ref[2 * r + n, pl.ds(my_slot // 2, 1), :]
            halves.append(jnp.where(xc == n, row, pltpu.roll(row, LANES // 2, 1)))
        tl_ref[r:r + 1] = jnp.where(lane1 < LANES // 2, halves[0], halves[1])


def fused(hidden, gamma, beta, valid, tgt, mask, embed):
    tok, dim = hidden.shape
    nc = 8
    own = tok // nc
    vb = embed.shape[0] // NB
    full = own * 8
    f32, bf16 = jnp.float32, jnp.bfloat16
    sds = jax.ShapeDtypeStruct
    vmem = pl.BlockSpec(memory_space=pltpu.VMEM)
    hbm = pl.BlockSpec(memory_space=pl.ANY)
    col = pltpu.VMEM((full, LANES), f32)
    coli = pltpu.VMEM((full, LANES), jnp.int32)
    dma, reg = pltpu.SemaphoreType.DMA, pltpu.SemaphoreType.REGULAR
    flops = 4 * full * nc * embed.shape[0] * dim
    return pl.pallas_call(
        fused_kernel,
        out_shape=(
            sds((NB, nc * full, vb), bf16),
            sds((nc, full, dim), bf16),
            sds((vb, dim), f32),
            sds((tok, dim), bf16),
            sds((nc // 2, LANES), f32),
            sds((8, dim), f32),
        ),
        in_specs=[vmem] * 6 + [hbm],
        out_specs=(hbm, hbm, hbm, vmem, vmem, vmem),
        scratch_shapes=[
            pltpu.VMEM((8, dim), f32),
            pltpu.VMEM((2, nc, LANES), f32),
            pltpu.VMEM((nc, 4, LANES), f32),
            pltpu.VMEM((nc, full, dim), bf16),
            pltpu.VMEM((NB, vb, dim), bf16),
            pltpu.VMEM((LAG, full, vb), f32),
            pltpu.VMEM((2, full, dim), f32),
            pltpu.VMEM((2, full, vb), bf16),
            pltpu.VMEM((NB, 1, vb), f32),
            col, col, col, coli, coli, col, col,
            pltpu.VMEM((8, 2, nc, LANES), f32),
            pltpu.VMEM((nc, 4, 8, LANES), f32),
            pltpu.VMEM((nc, 8, 4, 8, LANES), f32),
            pltpu.VMEM((2, full // 2, dim), f32),
            pltpu.VMEM((2, 2, own, dim), f32),
            pltpu.VMEM((2, own, dim), f32),
            pltpu.VMEM((8, dim), f32),
            pltpu.VMEM((8, 8, dim), f32),
            dma((NB,)), dma((nc, 4)), dma((nc, 7)), dma((nc, 3)), dma((8,)), dma((8,)), dma((nc, 8)), dma((nc, 8)),
            dma((2,)), dma((2,)), dma((2, 2)), dma((2, 2)), dma((2,)), dma((2,)),
            reg, reg, reg, dma((8,)), dma((8,)), dma((2,)), dma((nc,)), dma((2,)), dma((4,)),
        ],
        compiler_params=pltpu.CompilerParams(collective_id=0, has_side_effects=True, vmem_limit_bytes=67043328),
        cost_estimate=pl.CostEstimate(flops=flops, bytes_accessed=100_000_000, transcendentals=0),
    )(hidden, gamma, beta, valid, tgt, mask, embed.reshape(NB, vb, dim))


def grad_kernel(dz_ref, x_hbm, de_in, dh_in, tl_in, gb_in, o_hbm, dh_ref, tl_ref, dg_ref, db_ref, ml_ref, xbuf, obuf, ebuf, x_sem, o_sem, e_sem):
    s = pl.program_id(0)
    steps = pl.num_programs(0)
    parts, depth, _ = xbuf.shape
    mb = obuf.shape[1]
    edge = ebuf.shape[0]
    slot = lax.rem(s, 2)
    tn = (((0,), (0,)), ((), ()))

    def x_copy(n):
        return pltpu.make_async_copy(x_hbm.at[n], xbuf.at[n], x_sem.at[n])

    def out_copy(t):
        a = lax.rem(t, 2)
        return pltpu.make_async_copy(obuf.at[a], o_hbm.at[pl.ds(pl.multiple_of(edge + t * mb, mb), mb)], o_sem.at[a])

    e_in = pltpu.make_async_copy(de_in, ebuf, e_sem.at[0])
    e_out = pltpu.make_async_copy(ebuf, o_hbm.at[pl.ds(0, edge)], e_sem.at[1])

    @pl.when(s == 0)
    def _():
        for n in range(parts):
            x_copy(n).start()
        dh_ref[...] = dh_in[...]
        tl_ref[...] = tl_in[...]
        for r in range(dg_ref.shape[0]):
            dg_ref[r:r + 1] = gb_in[0:1, r * LANES:(r + 1) * LANES]
            db_ref[r:r + 1] = gb_in[1:2, r * LANES:(r + 1) * LANES]
        ml_ref[...] = gb_in[2:3, 0:1]
        for n in range(parts):
            x_copy(n).wait()
            part = lax.dot_general(dz_ref[pl.ds(n * depth, depth)], xbuf[n], tn, preferred_element_type=jnp.float32)
            if n == 0:
                obuf[0] = part
            else:
                obuf[0] += part
        e_in.start()

    @pl.when(s > 0)
    def _():
        @pl.when(s >= 2)
        def _():
            out_copy(s - 2).wait()

        @pl.when(s == 2)
        def _():
            e_in.wait()
            e_out.start()
        obuf[slot] = lax.dot_general(dz_ref[...], xbuf[...].reshape(parts * depth, -1), tn, preferred_element_type=jnp.float32)

    out_copy(s).start()

    @pl.when(s == steps - 1)
    def _():
        e_out.wait()
        out_copy(s - 1).wait()
        out_copy(s).wait()


def embed_grad(dz, x, de, d_hidden, tl, gb):
    nb, toks, vb = dz.shape
    dim = x.shape[-1]
    mb = vb // 2
    parts = 4
    f32 = jnp.float32
    sds = jax.ShapeDtypeStruct
    hbm = pl.BlockSpec(memory_space=pl.ANY)
    dma = pltpu.SemaphoreType.DMA

    def whole(shape):
        return pl.BlockSpec(shape, lambda s: (0, 0), pipeline_mode=pl.Buffered(1))

    return pl.pallas_call(
        grad_kernel,
        grid=((nb - 1) * 2,),
        out_shape=(
            sds((nb * vb, dim), f32), sds(d_hidden.shape, d_hidden.dtype), sds(tl.shape, f32),
            sds((dim // LANES, LANES), f32), sds((dim // LANES, LANES), f32), sds((1, 1), f32),
        ),
        in_specs=[
            pl.BlockSpec((None, toks, mb), lambda s: (1 + s // 2, 0, s % 2)),
            hbm, hbm, whole(d_hidden.shape), whole(tl.shape), whole(gb.shape),
        ],
        out_specs=(
            hbm,
            whole(d_hidden.shape), whole(tl.shape), whole((dim // LANES, LANES)), whole((dim // LANES, LANES)), whole((1, 1)),
        ),
        scratch_shapes=[
            pltpu.VMEM((parts, toks // parts, dim), x.dtype),
            pltpu.VMEM((2, mb, dim), f32),
            pltpu.VMEM((vb, dim), f32),
            dma((parts,)), dma((2,)), dma((2,)),
        ],
        compiler_params=pltpu.CompilerParams(vmem_limit_bytes=62 * 1024 * 1024),
        cost_estimate=pl.CostEstimate(flops=2 * toks * nb * vb * dim, bytes_accessed=100_000_000, transcendentals=0),
    )(dz, x.reshape(parts, toks // parts, dim), de, d_hidden, tl, gb)


def solution(mesh):
    tok_spec = P(("dp", "tp"))
    row_spec = P(("dp", "tp"), None)

    def local_step(hidden, gamma, beta, embed, valid, tgt, mask):
        tok, dim = hidden.shape
        def rows(v):
            return v.reshape(-1, LANES)

        dz, x_all, de, d_hidden, tl, gb = fused(hidden, rows(gamma), rows(beta), rows(valid), rows(tgt), rows(mask), embed)
        d_embed, d_hidden, tl, dg, db, ml = embed_grad(dz, x_all.reshape(-1, dim), de, d_hidden, tl, gb)
        return tl.reshape(-1), ml.reshape(1), d_hidden, d_embed, dg.reshape(-1), db.reshape(-1)

    return jax.shard_map(
        local_step,
        mesh=mesh,
        in_specs=(row_spec, P(), P(), P("tp", None), P("tp"), tok_spec, tok_spec),
        out_specs=(tok_spec, P("dp"), row_spec, row_spec, P("dp"), P("dp")),
        check_vma=False,
    )
```

```python
import functools

import jax
import jax.numpy as jnp
from jax import lax
from jax.experimental import pallas as pl
from jax.experimental.pallas import tpu as pltpu
from jax.sharding import PartitionSpec as P

LN_EPS = 1e-5
LANES = 128
NB = 5
AHEAD = 3
LAG = NB + 1
LOW = float(jnp.finfo(jnp.float32).min)
MESH = pl.DeviceIdType.MESH
NT = (((1,), (1,)), ((), ()))


def _spread(row):
    return jnp.broadcast_to(row, (LANES, LANES)).T


def fused_kernel(
    hid_ref, gam_in, bet_in, valid_in, tgt_in, mask_in, emb_hbm,
    dz_hbm, xall_hbm, de_hbm, dh_ref, tl_ref, gb_ref,
    par_ref, tm_src, loss_ref, xv, ev, ring, acc, dzb, bias, m_sc, s_sc, p_sc, t1_sc, t2_sc, lse_sc, w_sc,
    tm_all, st_send, st_recv, r0, r1, r2, gb_send, gb_recv,
    e_sem, ag_send, ag_recv, fw_send, tm_send, tm_recv, st_ssem, st_rsem,
    s0, q0, s1, q1, s2, q2, free0, free1, free2, gb_ssem, gb_rsem, dz_sem, x_sem, fz_sem, de_sem,
):
    nc, tok, dim = xv.shape
    vb = ev.shape[1]
    own = tok // 8
    half = tok // 2
    me = lax.axis_index("tp")
    core = lax.rem(me, 2)
    xc = lax.rem(me // 2, 2)
    yc = me // 4

    def dev(y, x, k):
        return y * 4 + x * 2 + k

    def slot_of(y, x, k):
        return k * 4 + y * 2 + x

    sib = dev(yc, xc, 1 - core)
    xn = dev(yc, 1 - xc, core)
    yn = dev(1 - yc, xc, core)
    dn = dev(1 - yc, 1 - xc, core)
    remote = ((xn, slot_of(yc, 1 - xc, core)), (yn, slot_of(1 - yc, xc, core)), (dn, slot_of(1 - yc, 1 - xc, core)))
    my_slot = slot_of(yc, xc, core)
    first_n = jnp.where(core == 0, xn, yn)
    second_n = jnp.where(core == 0, yn, xn)

    def rcopy(src, dst, ssem, rsem, to):
        return pltpu.make_async_remote_copy(src_ref=src, dst_ref=dst, send_sem=ssem, recv_sem=rsem, device_id={"tp": to}, device_id_type=MESH)

    def rows(slot):
        return pl.ds(pl.multiple_of(slot * own, own), own)

    for j in range(NB):
        pltpu.make_async_copy(emb_hbm.at[j], ev.at[j], e_sem.at[j]).start()

    barrier = pltpu.get_barrier_semaphore()
    for k in range(1, 8):
        pl.semaphore_signal(barrier, inc=1, device_id={"tp": lax.rem(me + k, 8)}, device_id_type=MESH)

    lane1 = lax.broadcasted_iota(jnp.int32, (1, LANES), 1)
    mine = (lane1 >= LANES // 2) == (xc == 1)
    for i, ref in enumerate((tgt_in, mask_in)):
        for c in range(nc):
            row = ref[c // 2:c // 2 + 1].astype(jnp.float32)
            row = jnp.where(xc == c % 2, row, pltpu.roll(row, LANES // 2, 1))
            tm_src[i, c:c + 1] = jnp.where(mine, row, 0.0)
    for r in range(dim // LANES):
        par_ref[0:1, pl.ds(r * LANES, LANES)] = gam_in[r:r + 1]
        par_ref[1:2, pl.ds(r * LANES, LANES)] = bet_in[r:r + 1]
    tm_all[me] = tm_src[...]

    def tm_copy(k):
        return rcopy(tm_src, tm_all.at[me], tm_send.at[k], tm_recv.at[k], lax.rem(me + k, 8))

    def ln(c):
        h = hid_ref[pl.ds(pl.multiple_of(c * own, own), own), :].astype(jnp.float32)
        cen = h - jnp.mean(h, axis=1, keepdims=True)
        rstd = lax.rsqrt(jnp.mean(cen * cen, axis=1, keepdims=True) + LN_EPS)
        return cen * rstd, rstd

    def ag_copy(c, k):
        r = xv.at[c, rows(my_slot)]
        return rcopy(r, r, ag_send.at[c, k], ag_recv.at[c, k], (xn, yn, dn, sib)[k])

    def fw_copy(c, k):
        r = xv.at[c, rows(remote[k][1])]
        return rcopy(r, r, fw_send.at[c, k], ag_recv.at[c, 4 + k], sib)

    def ag_start(c):
        for k in (2, 0, 1, 3):
            ag_copy(c, k).start()

    def ln_store(c):
        xhat, _ = ln(c)
        xv[c, rows(my_slot), :] = (xhat * par_ref[0:1] + par_ref[1:2]).astype(jnp.bfloat16)

    for c in range(2):
        ln_store(c)
    pl.semaphore_wait(barrier, 7)
    ag_start(0)
    for k in range(1, 8):
        tm_copy(k).start()

    def ln_body(c, _):
        ln_store(c)

        @pl.when(c <= AHEAD)
        def _():
            ag_start(c - 1)
        return 0

    lax.fori_loop(2, nc, ln_body, 0)
    for r in range(NB * vb // LANES):
        col = pl.ds(r % (vb // LANES) * LANES, LANES)
        bias[r // (vb // LANES), :, col] = jnp.where(valid_in[r:r + 1] > 0, 0.0, -jnp.inf)
    gb_send[...] = jnp.zeros_like(gb_send)

    def recv_remote(c):
        for k in range(3):
            ag_copy(c, k).wait_recv()

    def forward(c):
        recv_remote(c)
        for k in range(3):
            fw_copy(c, k).start()

    for k in range(1, 8):
        tm_copy(k).wait_recv()
    count = jnp.zeros((8, LANES), jnp.float32)
    for d in range(8):
        count = count + tm_all[d, 1]
    count = jnp.sum(jnp.sum(count, axis=1, keepdims=True), axis=0, keepdims=True)
    inv_n = 1.0 / count

    def tm_rows(c, which):
        out = []
        for q in range(4):
            k, y = q // 2, q % 2
            out.append(tm_all[dev(y, 0, k), which, pl.ds(c, 1), :] + tm_all[dev(y, 1, k), which, pl.ds(c, 1), :])
        return out

    forward(0)
    lane = lax.broadcasted_iota(jnp.int32, (tok, LANES), 1)

    def st_copy(c, k):
        return rcopy(st_send.at[c], st_recv.at[c, me], st_ssem.at[c, k], st_rsem.at[c, k], lax.rem(me + k, 8))

    def send_stats(c):
        for q in range(4):
            r = pl.ds(q * LANES, LANES)
            m = m_sc[r].T
            mx = jnp.max(m, axis=0, keepdims=True)
            st_send[c, q, 0:1] = mx
            st_send[c, q, 1:2] = jnp.sum(s_sc[r].T * jnp.exp(m - mx), axis=0, keepdims=True)
            st_send[c, q, 2:3] = jnp.sum(p_sc[r].T, axis=0, keepdims=True)
        st_recv[c, me] = st_send[c]
        for k in range(1, 8):
            st_copy(c, k).start()

    def use_stats(c):
        for k in range(1, 8):
            st_copy(c, k).wait_recv()
        tg = tm_rows(c, 0)
        mk = tm_rows(c, 1)
        for q in range(4):
            mx = st_recv[c, 0, q, 0:1]
            for d in range(1, 8):
                mx = jnp.maximum(mx, st_recv[c, d, q, 0:1])
            s = jnp.zeros_like(mx)
            p = jnp.zeros_like(mx)
            for d in range(8):
                s = s + st_recv[c, d, q, 1:2] * jnp.exp(st_recv[c, d, q, 0:1] - mx)
                p = p + st_recv[c, d, q, 2:3]
            lse = mx + jnp.log(s)
            loss_ref[c, pl.ds(q, 1), :] = (lse - p) * mk[q]
            w = mk[q] * inv_n
            r = pl.ds(q * LANES, LANES)
            lse_sc[r] = _spread(lse - jnp.log(w))
            w_sc[r] = _spread(w)
            t2_sc[r] = _spread(tg[q]).astype(jnp.int32)

    def begin_chunk(c):
        for k in range(3, 7):
            if k == 3:
                ag_copy(c, 3).wait_recv()
            else:
                fw_copy(c, k - 4).wait_recv()
        pltpu.make_async_copy(xv.at[c], xall_hbm.at[c], x_sem.at[c]).start()
        for n in range(2):
            @pl.when((c >= 1) & (AHEAD + 2 * (c - 1) + n < nc))
            def _(n=n):
                ag_start(AHEAD + 2 * (c - 1) + n)
        m_sc[...] = jnp.full(m_sc.shape, LOW, jnp.float32)
        s_sc[...] = jnp.zeros_like(s_sc)
        p_sc[...] = jnp.zeros_like(p_sc)
        tg = tm_rows(c, 0)
        for q in range(4):
            t1_sc[pl.ds(q * LANES, LANES)] = _spread(tg[q]).astype(jnp.int32)

    def first_src(b):
        return jnp.where(core == 0, b * 2 + (1 - xc), (1 - yc) * 2 + b)

    def first_keep(b):
        return jnp.where(core == 0, b * 2 + xc, yc * 2 + b)

    own2 = jnp.where(core == 0, yc, xc)

    def c0(c):
        a = lax.rem(c, 2)
        return rcopy(acc.at[a, pl.ds(pl.multiple_of((1 - core) * half, half), half)], r0.at[a], s0.at[a], q0.at[a], sib)

    def c1(c, b):
        a = lax.rem(c, 2)
        return rcopy(r0.at[a, rows(first_src(b))], r1.at[a, b], s1.at[a, b], q1.at[a, b], first_n)

    def c2(c):
        a = lax.rem(c, 2)
        return rcopy(r1.at[a, 1 - own2], r2.at[a], s2.at[a], q2.at[a], second_n)

    def stage0(c):
        @pl.when(c >= 2)
        def _():
            pl.semaphore_wait(free0, 1)
        c0(c).start()

    def stage1(c):
        a = lax.rem(c, 2)
        c0(c).wait()
        r0[a] = r0[a] + acc[a, pl.ds(pl.multiple_of(core * half, half), half)]

        @pl.when(c >= 2)
        def _():
            pl.semaphore_wait(free1, 1)
        for b in range(2):
            c1(c, b).start()

    def stage2(c):
        a = lax.rem(c, 2)
        for b in range(2):
            c1(c, b).wait()
        for b in range(2):
            r1[a, b] = r1[a, b] + r0[a, rows(first_keep(b))]

        @pl.when(c >= 2)
        def _():
            pl.semaphore_wait(free2, 1)
        c2(c).start()

        @pl.when(c < nc - 2)
        def _():
            pl.semaphore_signal(free0, inc=1, device_id={"tp": sib}, device_id_type=MESH)

    def stage3(c):
        a = lax.rem(c, 2)
        c2(c).wait()
        dy = r1[a, own2] + r2[a]

        @pl.when(c < nc - 2)
        def _():
            pl.semaphore_signal(free1, inc=1, device_id={"tp": first_n}, device_id_type=MESH)
            pl.semaphore_signal(free2, inc=1, device_id={"tp": second_n}, device_id_type=MESH)
        xhat, rstd = ln(c)
        gb_send[0:1] += jnp.sum(dy * xhat, axis=0, keepdims=True)
        gb_send[1:2] += jnp.sum(dy, axis=0, keepdims=True)
        dxh = dy * par_ref[0:1]
        m1 = jnp.mean(dxh, axis=1, keepdims=True)
        m2 = jnp.mean(dxh * xhat, axis=1, keepdims=True)
        dh_ref[pl.ds(pl.multiple_of(c * own, own), own), :] = (rstd * (dxh - m1 - xhat * m2)).astype(jnp.bfloat16)

    base = me * (NB * vb)

    def dz_copy(t):
        a = lax.rem(t, 2)
        t2 = t - LAG
        return pltpu.make_async_copy(dzb.at[a], dz_hbm.at[lax.rem(t2, NB), pl.ds(pl.multiple_of((t2 // NB) * tok, tok), tok)], dz_sem.at[a])

    def compute(t, do1, do2):
        slot = lax.rem(t, LAG)
        a2 = lax.rem(t, 2)
        cut = (vb // LANES + 1) // 4 * 2 * LANES if vb % 256 else (vb // 256 + 1) // 2 * 256
        pieces = ((0, cut), (cut, vb))
        j1 = lax.rem(t, NB)
        zs = []
        if do2:
            t2 = t - LAG
            j2 = lax.rem(t2, NB)
            a = lax.rem(t2 // NB, 2)
            tr2 = t2_sc[...] - (base + j2 * vb)
        for lo, hi in pieces:
            if do2:
                for col in range(lo, hi, LANES):
                    p = jnp.exp(ring[slot, :, pl.ds(col, LANES)] - lse_sc[...])
                    p = p - jnp.where(tr2 == lane + col, w_sc[...], 0.0)
                    dzb[a2, :, pl.ds(col, LANES)] = p.astype(jnp.bfloat16)
            if do1:
                zs.append(lax.dot_general(xv[t // NB], ev[j1, pl.ds(lo, hi - lo), :], NT, preferred_element_type=jnp.float32))
        if do1:
            tr1 = t1_sc[...] - (base + j1 * vb)
        for n, (lo, hi) in enumerate(pieces):
            w = pl.ds(lo, hi - lo)
            if do2:
                acc[a, :, pl.ds(lo * dim // vb, (hi - lo) * dim // vb)] += jnp.dot(
                    dzb[a2], ev[j2, :, pl.ds(lo * dim // vb, (hi - lo) * dim // vb)], preferred_element_type=jnp.float32)
            if do1:
                z = zs[n] + bias[j1, :, w]
                ring[slot, :, w] = z
                cols = [z[:, k * LANES:(k + 1) * LANES] for k in range((hi - lo) // LANES)]
                m0 = m_sc[...]
                m = m0
                for q in cols:
                    m = jnp.maximum(m, q)
                s = s_sc[...] * jnp.exp(m0 - m)
                pk = p_sc[...]
                for k, q in enumerate(cols):
                    s = s + jnp.exp(q - m)
                    pk = pk + jnp.where(tr1 == lane + (lo + k * LANES), q, 0.0)
                m_sc[...] = m
                s_sc[...] = s
                p_sc[...] = pk

    def step(t, do1, do2):
        ph = lax.rem(t, NB)
        per = t // NB

        @pl.when(ph == 0)
        def _():
            if do1:
                begin_chunk(per)
            if do2:
                @pl.when(t >= 15)
                def _():
                    stage2(per - 3)

        if do2:
            @pl.when(ph == 1)
            def _():
                @pl.when(t >= 11)
                def _():
                    stage0(per - 2)
                c = per - 1
                use_stats(c)
                acc[lax.rem(c, 2)] = jnp.zeros((tok, dim), jnp.float32)

        @pl.when(ph == 2)
        def _():
            if do1:
                @pl.when(per + 1 < nc)
                def _():
                    forward(per + 1)
            if do2:
                @pl.when(t >= 12)
                def _():
                    stage1(per - 2)

                @pl.when(t >= 17)
                def _():
                    stage3(per - 3)

        if do1:
            @pl.when(t < NB)
            def _():
                pltpu.make_async_copy(emb_hbm.at[ph], ev.at[ph], e_sem.at[ph]).wait()
        if do2:
            @pl.when(t >= LAG + 2)
            def _():
                dz_copy(t - 2).wait()
        compute(t, do1, do2)
        if do2:
            dz_copy(t).start()
        if do1:
            @pl.when(ph == NB - 1)
            def _():
                send_stats(t // NB)

    def loop(lo, hi, do1, do2):
        def body(t, _):
            step(t, do1, do2)
            return 0
        lax.fori_loop(lo, hi, body, 0)

    spans = [(n, lo, min(tok, vb - lo)) for n, lo in enumerate(range(0, vb, tok))]

    def fz_copy(c):
        a = lax.rem(c, 2)
        return pltpu.make_async_copy(dz_hbm.at[0, pl.ds(pl.multiple_of(c * tok, tok), tok)], dzb.at[a], fz_sem.at[a])

    def de_copy(n, lo, size):
        return pltpu.make_async_copy(ring.at[n, pl.ds(0, size)], de_hbm.at[pl.ds(lo, size)], de_sem.at[n])

    last = nc - 1

    def fill(f, _):
        @pl.when(f == 0)
        def _():
            stage0(last)
            for n, lo, size in spans:
                ring[n, :size] = jnp.zeros((size, dim), jnp.float32)

        @pl.when(f == 1)
        def _():
            stage1(last)

        @pl.when(f == 2)
        def _():
            stage3(last - 1)

        @pl.when(f == nc - 2)
        def _():
            stage2(last)
        fz_copy(f).wait()
        a = lax.rem(f, 2)
        for n, lo, size in spans:
            ring[n, :size] += lax.dot_general(dzb[a, :, pl.ds(lo, size)], xv[f], (((0,), (0,)), ((), ())), preferred_element_type=jnp.float32)

        @pl.when(f + 2 < nc)
        def _():
            fz_copy(f + 2).start()
        return 0

    total = NB * nc
    loop(0, LAG, True, False)
    loop(LAG, total, True, True)
    loop(total, total + LAG, False, True)
    for c in range(2):
        dz_copy(total + LAG - 2 + c).wait()
        fz_copy(lax.rem(total + LAG + c, 2)).start()
    lax.fori_loop(0, nc, fill, 0)
    for span in spans:
        de_copy(*span).start()
    stage3(last)

    def gb_copy(k):
        return rcopy(gb_send, gb_recv.at[me], gb_ssem.at[k], gb_rsem.at[k], lax.rem(me + k, 8))

    for k in range(1, 8):
        gb_copy(k).start()
    gb_recv[me] = gb_send[...]
    for span in spans:
        de_copy(*span).wait()

    def drain(c, _):
        for k in range(4):
            ag_copy(c, k).wait_send()
        for k in range(3):
            fw_copy(c, k).wait_send()
        for k in range(1, 8):
            st_copy(c, k).wait_send()
        pltpu.make_async_copy(xv.at[c], xall_hbm.at[c], x_sem.at[c]).wait()
        return 0

    lax.fori_loop(0, nc, drain, 0)
    for k in range(1, 8):
        tm_copy(k).wait_send()
        gb_copy(k).wait()
    tot = gb_recv[0]
    for d in range(1, 8):
        tot = tot + gb_recv[d]
    gb_ref[...] = tot
    mean = jnp.zeros((4, LANES), jnp.float32)
    for c in range(nc):
        mean = mean + loss_ref[c]
    mean = jnp.sum(jnp.sum(mean, axis=1, keepdims=True), axis=0, keepdims=True) / count
    gb_ref[2:3] = jnp.broadcast_to(mean, (1, dim))
    for r in range(nc // 2):
        halves = []
        for n in range(2):
            row = loss_ref[2 * r + n, pl.ds(my_slot // 2, 1), :]
            halves.append(jnp.where(xc == n, row, pltpu.roll(row, LANES // 2, 1)))
        tl_ref[r:r + 1] = jnp.where(lane1 < LANES // 2, halves[0], halves[1])


def fused(hidden, gamma, beta, valid, tgt, mask, embed):
    tok, dim = hidden.shape
    nc = 8
    own = tok // nc
    vb = embed.shape[0] // NB
    full = own * 8
    f32, bf16 = jnp.float32, jnp.bfloat16
    sds = jax.ShapeDtypeStruct
    vmem = pl.BlockSpec(memory_space=pltpu.VMEM)
    hbm = pl.BlockSpec(memory_space=pl.ANY)
    col = pltpu.VMEM((full, LANES), f32)
    coli = pltpu.VMEM((full, LANES), jnp.int32)
    dma, reg = pltpu.SemaphoreType.DMA, pltpu.SemaphoreType.REGULAR
    flops = 4 * full * nc * embed.shape[0] * dim
    return pl.pallas_call(
        fused_kernel,
        out_shape=(
            sds((NB, nc * full, vb), bf16),
            sds((nc, full, dim), bf16),
            sds((vb, dim), f32),
            sds((tok, dim), bf16),
            sds((nc // 2, LANES), f32),
            sds((8, dim), f32),
        ),
        in_specs=[vmem] * 6 + [hbm],
        out_specs=(hbm, hbm, hbm, vmem, vmem, vmem),
        scratch_shapes=[
            pltpu.VMEM((8, dim), f32),
            pltpu.VMEM((2, nc, LANES), f32),
            pltpu.VMEM((nc, 4, LANES), f32),
            pltpu.VMEM((nc, full, dim), bf16),
            pltpu.VMEM((NB, vb, dim), bf16),
            pltpu.VMEM((LAG, full, vb), f32),
            pltpu.VMEM((2, full, dim), f32),
            pltpu.VMEM((2, full, vb), bf16),
            pltpu.VMEM((NB, 1, vb), f32),
            col, col, col, coli, coli, col, col,
            pltpu.VMEM((8, 2, nc, LANES), f32),
            pltpu.VMEM((nc, 4, 8, LANES), f32),
            pltpu.VMEM((nc, 8, 4, 8, LANES), f32),
            pltpu.VMEM((2, full // 2, dim), f32),
            pltpu.VMEM((2, 2, own, dim), f32),
            pltpu.VMEM((2, own, dim), f32),
            pltpu.VMEM((8, dim), f32),
            pltpu.VMEM((8, 8, dim), f32),
            dma((NB,)), dma((nc, 4)), dma((nc, 7)), dma((nc, 3)), dma((8,)), dma((8,)), dma((nc, 8)), dma((nc, 8)),
            dma((2,)), dma((2,)), dma((2, 2)), dma((2, 2)), dma((2,)), dma((2,)),
            reg, reg, reg, dma((8,)), dma((8,)), dma((2,)), dma((nc,)), dma((2,)), dma((4,)),
        ],
        compiler_params=pltpu.CompilerParams(collective_id=0, has_side_effects=True, vmem_limit_bytes=67043328),
        cost_estimate=pl.CostEstimate(flops=flops, bytes_accessed=100_000_000, transcendentals=0),
    )(hidden, gamma, beta, valid, tgt, mask, embed.reshape(NB, vb, dim))


def grad_kernel(dz_ref, x_hbm, de_in, dh_in, tl_in, gb_in, o_hbm, dh_ref, tl_ref, dg_ref, db_ref, ml_ref, xbuf, obuf, ebuf, x_sem, o_sem, e_sem):
    s = pl.program_id(0)
    steps = pl.num_programs(0)
    parts, depth, _ = xbuf.shape
    mb = obuf.shape[1]
    edge = ebuf.shape[0]
    slot = lax.rem(s, 2)
    tn = (((0,), (0,)), ((), ()))

    def x_copy(n):
        return pltpu.make_async_copy(x_hbm.at[n], xbuf.at[n], x_sem.at[n])

    def out_copy(t):
        a = lax.rem(t, 2)
        return pltpu.make_async_copy(obuf.at[a], o_hbm.at[pl.ds(pl.multiple_of(edge + t * mb, mb), mb)], o_sem.at[a])

    e_in = pltpu.make_async_copy(de_in, ebuf, e_sem.at[0])
    e_out = pltpu.make_async_copy(ebuf, o_hbm.at[pl.ds(0, edge)], e_sem.at[1])

    @pl.when(s == 0)
    def _():
        for n in range(parts):
            x_copy(n).start()
        dh_ref[...] = dh_in[...]
        tl_ref[...] = tl_in[...]
        for r in range(dg_ref.shape[0]):
            dg_ref[r:r + 1] = gb_in[0:1, r * LANES:(r + 1) * LANES]
            db_ref[r:r + 1] = gb_in[1:2, r * LANES:(r + 1) * LANES]
        ml_ref[...] = gb_in[2:3, 0:1]
        for n in range(parts):
            x_copy(n).wait()
            part = lax.dot_general(dz_ref[pl.ds(n * depth, depth)], xbuf[n], tn, preferred_element_type=jnp.float32)
            if n == 0:
                obuf[0] = part
            else:
                obuf[0] += part
        e_in.start()

    @pl.when(s > 0)
    def _():
        @pl.when(s >= 2)
        def _():
            out_copy(s - 2).wait()

        @pl.when(s == 2)
        def _():
            e_in.wait()
            e_out.start()
        obuf[slot] = lax.dot_general(dz_ref[...], xbuf[...].reshape(parts * depth, -1), tn, preferred_element_type=jnp.float32)

    out_copy(s).start()

    @pl.when(s == steps - 1)
    def _():
        e_out.wait()
        out_copy(s - 1).wait()
        out_copy(s).wait()


def embed_grad(dz, x, de, d_hidden, tl, gb):
    nb, toks, vb = dz.shape
    dim = x.shape[-1]
    mb = vb // 2
    parts = 4
    f32 = jnp.float32
    sds = jax.ShapeDtypeStruct
    hbm = pl.BlockSpec(memory_space=pl.ANY)
    dma = pltpu.SemaphoreType.DMA

    def whole(shape):
        return pl.BlockSpec(shape, lambda s: (0, 0), pipeline_mode=pl.Buffered(1))

    return pl.pallas_call(
        grad_kernel,
        grid=((nb - 1) * 2,),
        out_shape=(
            sds((nb * vb, dim), f32), sds(d_hidden.shape, d_hidden.dtype), sds(tl.shape, f32),
            sds((dim // LANES, LANES), f32), sds((dim // LANES, LANES), f32), sds((1, 1), f32),
        ),
        in_specs=[
            pl.BlockSpec((None, toks, mb), lambda s: (1 + s // 2, 0, s % 2)),
            hbm, hbm, whole(d_hidden.shape), whole(tl.shape), whole(gb.shape),
        ],
        out_specs=(
            hbm,
            whole(d_hidden.shape), whole(tl.shape), whole((dim // LANES, LANES)), whole((dim // LANES, LANES)), whole((1, 1)),
        ),
        scratch_shapes=[
            pltpu.VMEM((parts, toks // parts, dim), x.dtype),
            pltpu.VMEM((2, mb, dim), f32),
            pltpu.VMEM((vb, dim), f32),
            dma((parts,)), dma((2,)), dma((2,)),
        ],
        compiler_params=pltpu.CompilerParams(vmem_limit_bytes=62 * 1024 * 1024),
        cost_estimate=pl.CostEstimate(flops=2 * toks * nb * vb * dim, bytes_accessed=100_000_000, transcendentals=0),
    )(dz, x.reshape(parts, toks // parts, dim), de, d_hidden, tl, gb)


def solution(mesh):
    tok_spec = P(("dp", "tp"))
    row_spec = P(("dp", "tp"), None)

    def local_step(hidden, gamma, beta, embed, valid, tgt, mask):
        tok, dim = hidden.shape
        def rows(v):
            return v.reshape(-1, LANES)

        dz, x_all, de, d_hidden, tl, gb = fused(hidden, rows(gamma), rows(beta), rows(valid), rows(tgt), rows(mask), embed)
        d_embed, d_hidden, tl, dg, db, ml = embed_grad(dz, x_all.reshape(-1, dim), de, d_hidden, tl, gb)
        return tl.reshape(-1), ml.reshape(1), d_hidden, d_embed, dg.reshape(-1), db.reshape(-1)

    return jax.shard_map(
        local_step,
        mesh=mesh,
        in_specs=(row_spec, P(), P(), P("tp", None), P("tp"), tok_spec, tok_spec),
        out_specs=(tok_spec, P("dp"), row_spec, row_spec, P("dp"), P("dp")),
        check_vma=False,
    )
```
